1024 devices in a mesh: dp: 64 (over x_hi, z, core), tensor: 16 (over x_lo, y).
Axes of the slice: x: 4 (x_hi: 2, x_lo: 2; x = x_hi * 2 + x_lo), y: 8, z: 16, core: 2. Of those that a mesh axis runs over, the one named last changes fastest.
Arguments:
- block_input: bfloat16 [16384, 5120], P('dp'), may hold values from -16 to 16
- query_weight: bfloat16 [2560, 5120], P('tensor'), as said below
- query_gain: float32 [2560], P('tensor'), may hold values from 0.5 to 2
- query_grad: bfloat16 [2560, 16384], P('tensor', 'dp'), may hold values from -6 to 6
Outputs:
- input_grad: bfloat16 [16384, 5120], P(('dp', 'tensor'))
- weight_grad: float32 [5120, 2560], P('dp', 'tensor')
The draws below stay inside these ranges and needn't reach their ends.
Inputs may be any that keep to these rules, and one draw needn't show every extreme that they name: `query_weight`: entries are normal with standard deviation 5120 ** -0.5 times a factor between 0.25 and 75, which may differ from row to row and from column to column.
All inputs are finite; a program needn't handle non-finite values.
Results may differ from the reference program's by a relative error of at most 0.017.
Values may be sent and summed in bfloat16 or wider, within the bound.
A program may use at most 64 MiB of HBM per device.

```python
import math
import jax
import jax.numpy as jnp
from jax import lax

D = 5120
HQ = 2560
TOKENS = 16384
N_TENSOR = 16


def draw_query_weight(key, part):
    first = jax.random.fold_in(key, 0)
    base = jax.random.normal(first, (HQ, D), jnp.float32) / math.sqrt(D)
    ramp = jnp.exp(math.log(3.0) * jnp.arange(HQ, dtype=jnp.float32) / HQ)[:, None]
    return (base * ramp).astype(jnp.bfloat16)


def strengthened(values, stream_key, source, target, shards_of, factor):
    def block_of(dim):
        return (jnp.arange(values.shape[dim]) // (values.shape[dim] // shards_of)).reshape((-1,) + (1,) * (values.ndim - 1 - dim))

    first = jax.random.permutation(stream_key, shards_of)[block_of(target)]
    far = (block_of(target) + shards_of // 2) % shards_of
    return jnp.where((block_of(source) == first) | (block_of(source) == far), factor * values, values)


def block_levels(rng, extent, shards, least, high):
    factor_of, own = 1.0, jax.random.fold_in(rng, 6)
    for position, parts in shards:
        steps = jnp.exp(jax.random.uniform(jax.random.fold_in(own, position), (parts,), jnp.float32, least / len(shards), high / len(shards)))
        factor_of = factor_of * jnp.repeat(steps, extent[position] // parts).reshape([-1 if axis == position else 1 for axis in range(len(extent))])
    return factor_of


def centred(key, shape, deviation, limit, cuts=(), held_as=jnp.bfloat16):
    factor_of = block_levels(key, shape, cuts, -0.22, 0.18) if cuts else 1.0
    result = jax.random.normal(key, shape, jnp.float32) * deviation * factor_of
    return jnp.minimum(jnp.maximum(result, -limit), limit).astype(held_as)


def heavy_noise(stream_key, dims, scale, most, cuts, heavy, kind=jnp.bfloat16):
    values = scale * jax.random.normal(stream_key, dims, jnp.float32)
    if cuts:
        values = values * block_levels(stream_key, dims, cuts, -0.22, 0.18)
    return jnp.clip(strengthened(values, jax.random.fold_in(stream_key, 3), *heavy), -most, most).astype(kind)


def setup_inputs(seed: int = 0) -> dict:
    splits = jax.random.split(jax.random.key(seed), 5)
    return {
        "block_input": heavy_noise(splits[0], (TOKENS, D), 1.0, 16.0, ((0, 64),), (0, 1, 64, 4.0)),
        "query_weight": draw_query_weight(jax.random.fold_in(splits[4], 71), 0),
        "query_gain": jnp.clip(jnp.exp(math.log(2.0) - 1.3862944 * jax.random.uniform(splits[2], (HQ,), jnp.float32) ** block_levels(splits[2], (HQ,), ((0, 16),), -0.2, 0.2)), 0.5, 2.0),
        "query_grad": centred(splits[3], (HQ, TOKENS), 1.0, 6.0, ((0, 16), (1, 64))),
    }


epsilon = 1e-06

def reference(block_input, query_weight, query_gain, query_grad):
    projected = jnp.dot(block_input, query_weight.T, preferred_element_type=jnp.float32)
    squares = lax.optimization_barrier(jnp.sum(projected * projected, axis=1, keepdims=True))
    inverse_rms = 1.0 / jnp.sqrt(squares / HQ + epsilon)
    scaled_grad = query_grad.T.astype(jnp.float32) * query_gain
    cross_sums = lax.optimization_barrier(jnp.sum(scaled_grad * projected, axis=1, keepdims=True))
    coefficient = inverse_rms * inverse_rms * inverse_rms * (cross_sums / HQ)
    proj_grad = (inverse_rms * scaled_grad - coefficient * projected).astype(jnp.bfloat16)
    group = HQ // N_TENSOR
    total = jnp.zeros((TOKENS, D), jnp.float32)
    for member in range(N_TENSOR):
        lower = member * group
        term = jnp.dot(proj_grad[:, lower:lower + group], query_weight[lower:lower + group, :], preferred_element_type=jnp.float32)
        rounded = lax.optimization_barrier(term.astype(jnp.bfloat16)).astype(jnp.float32)
        total = total + rounded
    input_grad = total.astype(jnp.bfloat16)
    weight_grad = jnp.dot(block_input.T, proj_grad, preferred_element_type=jnp.float32)
    return (input_grad, weight_grad)
```

```python
import jax
import jax.numpy as jnp
from jax import lax
from jax.experimental import pallas as pl
from jax.experimental.pallas import tpu as pltpu
from jax.sharding import PartitionSpec as P

MESH = pl.DeviceIdType.MESH
F32, BF16 = jnp.float32, jnp.bfloat16

NT, NY, NZ = 16, 8, 16
T, F, D = 256, 160, 5120
HALF = D // 2
S = 4
CS = HALF // S
KC = 4
KW = D // KC
HQ = F * NT
epsilon = 1e-6

STEPS = ((8, 4, -7, -4), (7, 3, -6, -3), (6, 2, -5, -2), (5, 1, -1, 0))
LAST = {5: 0, 1: 1, -5: 2, -1: 3}
HEADS = (8, 4, -7, -4)
YSTEPS = ((4, -3), (3, -2), (2, -1), (1,))
YHEADS = (4, -3)

SUMS = 0
WX = SUMS + NT
WD = WX + 4
PG = WD + 4
DD = PG + 1
ZC = DD + 4
FIN = ZC + 16
YC = FIN + 9
YF = YC + 8 * S
NSEM = YF + S


def dot(a, b, dims):
    return lax.dot_general(a, b, (dims, ((), ())), preferred_element_type=F32)


def kernel(
    x_hbm, w_hbm, gain_ref, qg_hbm, ig_hbm, wg_hbm,
    x_v, xt_v, w_v, wh_v, wp_v, qg_v, sums_v, pga_v, pgb_v, pgp_v,
    dsend, drecv, own_v, zsend, zrecv, fin_v, wg_v,
    part_v, ysend, yrecv, yfin, yfinr,
    lsem, ssem, rsem,
):
    d = lax.axis_index("dp")
    t = lax.axis_index("tensor")
    core = lax.rem(d, 2)
    z = lax.rem(lax.div(d, 2), NZ)
    xh = lax.div(d, 2 * NZ)
    y = lax.rem(t, NY)
    xl = lax.div(t, NY)
    sgn = 1 - 2 * core

    def dev(xh_, z_, core_, xl_, y_):
        return {"dp": (xh_ * NZ + z_) * 2 + core_, "tensor": xl_ * NY + y_}

    def zat(r):
        return lax.rem(z + sgn * r + 2 * NZ, NZ)

    def yat(r):
        return lax.rem(y + sgn * r + 2 * NY, NY)

    sibling = dev(xh, z, 1 - core, xl, y)
    partner = dev(xh, z, core, 1 - xl, y)
    across = dev(1 - xh, z, core, 1 - xl, y)

    loads = []
    for k in range(KC):
        cols = pl.ds(k * KW, KW)
        loads.append((
            pltpu.make_async_copy(x_hbm.at[:, cols], x_v.at[:, cols], lsem.at[k]),
            pltpu.make_async_copy(w_hbm.at[:, cols], w_v.at[:, cols], lsem.at[KC + k]),
        ))
    for a, b in loads:
        a.start()
        b.start()
    qg_load = pltpu.make_async_copy(qg_hbm, qg_v, lsem.at[2 * KC])
    qg_load.start()
    myhalf = pl.ds(pl.multiple_of(xl * HALF, 128), HALF)
    wh_load = pltpu.make_async_copy(w_hbm.at[:, myhalf], wh_v, lsem.at[2 * KC + 1])
    wh_load.start()

    barrier = pltpu.get_barrier_semaphore()
    peers = [{"dp": d, "tensor": lax.rem(t + o, NT)} for o in range(1, NT)]
    peers += [across, sibling]
    peers += [dev(xh, zat(r), core, xl, y) for r in (1, -1, 5, -5)]
    peers += [dev(1 - xh, zat(r), core, xl, y) for r in (1, -1, 5, -5, 0)]
    for p in peers:
        pl.semaphore_signal(barrier, inc=1, device_id=p, device_id_type=MESH)

    pt = None
    for k, (a, b) in enumerate(loads):
        a.wait()
        b.wait()
        cols = slice(k * KW, (k + 1) * KW)
        term = dot(w_v[:, cols], x_v[:, cols], ((1,), (1,)))
        pt = term if pt is None else pt + term
    qg_load.wait()
    rows = lax.broadcasted_iota(jnp.int32, (F, F), 0)
    lanes = lax.broadcasted_iota(jnp.int32, (F, F), 1)
    gain = jnp.sum(jnp.where(rows == lanes, gain_ref[...], 0.0), axis=1, keepdims=True)
    sg = qg_v[...].astype(F32) * gain
    sq = jnp.sum(pt * pt, axis=0, keepdims=True)
    cr = jnp.sum(sg * pt, axis=0, keepdims=True)
    sums_v[t, 0:1, :] = sq[:, :128]
    sums_v[t, 1:2, :] = sq[:, 128:]
    sums_v[t, 2:3, :] = cr[:, :128]
    sums_v[t, 3:4, :] = cr[:, 128:]

    pl.semaphore_wait(barrier, len(peers))

    started = []

    def send(src, dst, index, device):
        copy = pltpu.make_async_remote_copy(
            src_ref=src, dst_ref=dst, send_sem=ssem.at[index], recv_sem=rsem.at[index],
            device_id=device, device_id_type=MESH,
        )
        copy.start()
        started.append(copy)

    def arrived(dst, index):
        pltpu.make_async_remote_copy(
            src_ref=dst, dst_ref=dst, send_sem=ssem.at[index], recv_sem=rsem.at[index],
            device_id=sibling, device_id_type=MESH,
        ).wait_recv()

    for o in range(1, NT):
        copy = pltpu.make_async_remote_copy(
            src_ref=sums_v.at[t], dst_ref=sums_v.at[t],
            send_sem=ssem.at[SUMS + o], recv_sem=rsem.at[SUMS + t],
            device_id=peers[o - 1], device_id_type=MESH,
        )
        copy.start()
        started.append(copy)

    for n, who in enumerate((partner, across)):
        src = pl.ds(pl.multiple_of((1 - xl) * HALF + (2 * n + core) * CS, 128), CS)
        dst = pl.ds(pl.multiple_of((2 * n + core) * CS, 128), CS)
        send(w_v.at[:, src], wp_v.at[:, dst], WX + n, who)

    for k in range(D // 256):
        xt_v[k * 256 : (k + 1) * 256, :] = x_v[:, k * 256 : (k + 1) * 256].T
    pga_v[F:, :] = jnp.zeros((256 - F, T), BF16)
    pgb_v[128:160, :] = jnp.zeros((32, T), BF16)
    pgb_v[192:, :] = jnp.zeros((64, T), BF16)

    for o in range(1, NT):
        s = lax.rem(t + o, NT)
        arrived(sums_v.at[s], SUMS + s)
    total = sums_v[0]
    for s in range(1, NT):
        total = total + sums_v[s]
    sq = jnp.concatenate([total[0:1], total[1:2]], axis=1)
    cr = jnp.concatenate([total[2:3], total[3:4]], axis=1)
    inv = 1.0 / jnp.sqrt(sq / HQ + epsilon)
    coef = inv * inv * inv * (cr / HQ)
    pg = (inv * sg - coef * pt).astype(BF16)
    pga_v[:F, :] = pg
    pgb_v[:128, :] = pg[:128]
    pgb_v[160:192, :] = pg[128:]
    send(pga_v.at[:F], pgp_v, PG, partner)

    def block(dest, who):
        out = []
        for h, rhs in ((0, pga_v), (1, pgb_v)):
            at = pl.multiple_of(h * HALF + dest * 160 + who * 80, 16)
            out.append(dot(xt_v[pl.ds(at, 80), :], rhs[...], ((1,), (1,))))
        return out[0][:, :128], out[0][:, 128:] + out[1][:, 128:], out[1][:, :128]

    def blocks(g):
        for i, r in enumerate(STEPS[g]):
            for j, v in enumerate(block(lax.rem(z - sgn * r + 2 * NZ, NZ), 1 - core)):
                dsend[g, i, j * 80 : (j + 1) * 80, :] = v.astype(BF16)
        send(dsend.at[g], drecv.at[g], DD + g, sibling)
        for i, r in enumerate(STEPS[g]):
            for j, v in enumerate(block(zat(r), core)):
                own_v[g, i, j * 80 : (j + 1) * 80, :] = v

    def zstep(g):
        arrived(drecv.at[g], DD + g)
        for i, r in enumerate(STEPS[g]):
            if r not in HEADS and r != 0:
                arrived(zrecv.at[r % NZ], ZC + r % NZ)
            v = own_v[g, i] + drecv[g, i].astype(F32)
            if r == 0:
                own_v[g, i] = v
                zsend[0] = v.astype(BF16)
                send(
                    zsend.at[0, pl.ds(pl.multiple_of((1 - xh) * 80, 16), 160)],
                    fin_v.at[8], FIN + 8, dev(1 - xh, z, core, xl, y),
                )
                continue
            if r not in HEADS:
                v = v + zrecv[r % NZ].astype(F32)
            zsend[r % NZ] = v.astype(BF16)
            if r in LAST:
                for flag, h in ((0, xh), (1, 1 - xh)):
                    slot = LAST[r] * 2 + flag
                    send(
                        zsend.at[r % NZ, pl.ds(pl.multiple_of(h * 80, 16), 160)],
                        fin_v.at[slot], FIN + slot, dev(h, zat(r), core, xl, y),
                    )
            else:
                nxt = r - 1 if r > 0 else r + 1
                send(
                    zsend.at[r % NZ], zrecv.at[nxt % NZ], ZC + nxt % NZ,
                    dev(xh, zat(1 if r > 0 else -1), core, xl, y),
                )

    def yrows(r):
        return pl.multiple_of(yat(r) * 16, 16)

    def ystep(k, s):
        for r in YSTEPS[k]:
            at = yrows(r)
            new = [part_v[s, pl.ds(at + h * 128, 16), :] for h in (0, 1)]
            slot = (r % NY) * S + s
            if r not in YHEADS:
                arrived(yrecv.at[r % NY, s], YC + slot)
                new = [v + yrecv[r % NY, s, h * 16 : h * 16 + 16, :].astype(F32) for h, v in enumerate(new)]
            for h, v in enumerate(new):
                ysend[r % NY, s, h * 16 : h * 16 + 16, :] = v.astype(BF16)
            nxt = r - 1 if r > 0 else r + 1
            to = nxt % NY if nxt else (0 if r > 0 else 4)
            send(
                ysend.at[r % NY, s], yrecv.at[to, s], YC + to * S + s,
                dev(xh, z, core, xl, yat(1 if r > 0 else -1)),
            )

    blocks(0)
    zstep(0)
    for g in (1, 2, 3):
        blocks(g)

    for n in (0, 1):
        cols = pl.ds(pl.multiple_of((2 * n + core) * CS, 128), CS)
        arrived(wp_v.at[:, cols], WX + n)
        send(wp_v.at[:, cols], wp_v.at[:, cols], WD + n, sibling)
    wh_load.wait()
    arrived(pgp_v, PG)
    for n in (0, 1):
        cols = pl.ds(pl.multiple_of((2 * n + 1 - core) * CS, 128), CS)
        arrived(wp_v.at[:, cols], WD + n)
    for s in range(S):
        cols = slice(s * CS, (s + 1) * CS)
        part_v[s] = dot(pga_v[:F, :], wh_v[:, cols], ((0,), (0,))) + dot(
            pgp_v[...], wp_v[:, cols], ((0,), (0,))
        )
        ystep(0, s)

    for k in (1, 2, 3):
        zstep(k)
        for s in range(S):
            ystep(k, s)

    outs = []
    for s in range(S):
        arrived(yrecv.at[0, s], YC + s)
        arrived(yrecv.at[4, s], YC + 4 * S + s)
        for h in (0, 1):
            rows = slice(h * 16, h * 16 + 16)
            v = part_v[s, pl.ds(yrows(0) + h * 128, 16), :]
            v = v + yrecv[0, s, rows, :].astype(F32) + yrecv[4, s, rows, :].astype(F32)
            yfin[s, rows, :] = v.astype(BF16)
        send(
            yfin.at[s, pl.ds(pl.multiple_of((1 - xl) * 16, 16), 16)], yfinr.at[s], YF + s, partner
        )
        copy = pltpu.make_async_copy(
            yfin.at[s, pl.ds(pl.multiple_of(xl * 16, 16), 16)],
            ig_hbm.at[:, pl.ds(pl.multiple_of(xl * HALF + s * CS, 128), CS)],
            lsem.at[2 * KC + 2 + s],
        )
        copy.start()
        outs.append(copy)

    for slot in range(9):
        arrived(fin_v.at[slot], FIN + slot)
    main_at = pl.multiple_of(xh * 80, 16)
    rest_at = pl.multiple_of((1 - xh) * 80, 16)
    main = own_v[3, 3, pl.ds(pl.multiple_of(xh * 160, 16), 80), :]
    rest = own_v[3, 3, 80:160, :]
    for slot in range(9):
        main = main + fin_v[slot, pl.ds(main_at, 80), :].astype(F32)
        rest = rest + fin_v[slot, pl.ds(rest_at, 80), :].astype(F32)
    wg_v[:, :128] = main
    wg_v[:, 128:] = jnp.where(xh == 0, rest[:, :32], rest[:, 32:64])
    wg_copy = pltpu.make_async_copy(wg_v, wg_hbm, lsem.at[2 * KC + 2 + 2 * S])
    wg_copy.start()
    outs.append(wg_copy)

    for s in range(S):
        arrived(yfinr.at[s], YF + s)
        copy = pltpu.make_async_copy(
            yfinr.at[s],
            ig_hbm.at[:, pl.ds(pl.multiple_of((1 - xl) * HALF + s * CS, 128), CS)],
            lsem.at[2 * KC + 2 + S + s],
        )
        copy.start()
        outs.append(copy)
    for copy in started:
        copy.wait_send()
    for copy in outs:
        copy.wait()


def per_device(block_input, query_weight, query_gain, query_grad):
    hbm = pl.BlockSpec(memory_space=pl.ANY)
    vmem = pl.BlockSpec(memory_space=pltpu.VMEM)
    return pl.pallas_call(
        kernel,
        out_shape=(
            jax.ShapeDtypeStruct((T // NT, D), BF16),
            jax.ShapeDtypeStruct((80, F), F32),
        ),
        in_specs=[hbm, hbm, vmem, hbm],
        out_specs=(hbm, hbm),
        scratch_shapes=[
            pltpu.VMEM((T, D), BF16),
            pltpu.VMEM((D, T), BF16),
            pltpu.VMEM((F, D), BF16),
            pltpu.VMEM((F, HALF), BF16),
            pltpu.VMEM((F, HALF), BF16),
            pltpu.VMEM((F, T), BF16),
            pltpu.VMEM((NT, 4, 128), F32),
            pltpu.VMEM((256, T), BF16),
            pltpu.VMEM((256, T), BF16),
            pltpu.VMEM((F, T), BF16),
            pltpu.VMEM((4, 4, 240, 128), BF16),
            pltpu.VMEM((4, 4, 240, 128), BF16),
            pltpu.VMEM((4, 4, 240, 128), F32),
            pltpu.VMEM((16, 240, 128), BF16),
            pltpu.VMEM((16, 240, 128), BF16),
            pltpu.VMEM((9, 160, 128), BF16),
            pltpu.VMEM((80, F), F32),
            pltpu.VMEM((S, T, CS), F32),
            pltpu.VMEM((8, S, 32, CS), BF16),
            pltpu.VMEM((8, S, 32, CS), BF16),
            pltpu.VMEM((S, 32, CS), BF16),
            pltpu.VMEM((S, 16, CS), BF16),
            pltpu.SemaphoreType.DMA((2 * KC + 3 + 2 * S,)),
            pltpu.SemaphoreType.DMA((NSEM,)),
            pltpu.SemaphoreType.DMA((NSEM,)),
        ],
        compiler_params=pltpu.CompilerParams(
            collective_id=0, has_side_effects=True, vmem_limit_bytes=40 * 1024 * 1024
        ),
    )(block_input, query_weight, query_gain.reshape(1, F), query_grad)


def solution(mesh):
    return jax.shard_map(
        per_device,
        mesh=mesh,
        in_specs=(P("dp", None), P("tensor", None), P("tensor"), P("tensor", "dp")),
        out_specs=(P(("dp", "tensor"), None), P("dp", "tensor")),
        check_vma=False,
    )
```

```python
import jax
import jax.numpy as jnp
from jax import lax
from jax.experimental import pallas as pl
from jax.experimental.pallas import tpu as pltpu
from jax.sharding import PartitionSpec as P

MESH = pl.DeviceIdType.MESH
F32, BF16 = jnp.float32, jnp.bfloat16

NT, NY, NZ = 16, 8, 16
T, F, D = 256, 160, 5120
HALF = D // 2
S = 4
CS = HALF // S
KC = 4
KW = D // KC
HQ = F * NT
epsilon = 1e-6

PARENT = {8: 7, 7: 5, 6: 5, 5: 0, 4: 3, 3: 1, 2: 1, 1: 0, -7: -5, -6: -5, -5: 0, -4: -3, -3: -1, -2: -1, -1: 0}
CROSS = {8: 7, 7: 7, 6: 5, 5: 5, 4: 3, 3: 3, 2: 1, 1: 1, 0: 0, -7: -5, -6: -5, -5: -5, -4: -3, -3: -3, -2: -1, -1: -1}
GROUPS = ((8, 7, -7), (6, -6, 5, -5), (4, -4, 3, -3), (2, -2, 1, -1, 0))
ORDER = sum(GROUPS, ())
AT = {r: i for i, r in enumerate(ORDER)}
STAGES = ((7, 3, -3), (5, -5, 1, -1))
JOINS = STAGES[0] + STAGES[1] + (0,)
SLOT, JOIN_SLOTS = {}, {}
for j in JOINS:
    first = len(SLOT)
    for r in ORDER:
        if PARENT.get(r) == j:
            SLOT["own", r] = len(SLOT)
        if CROSS[r] == j:
            SLOT["cross", r] = len(SLOT)
    JOIN_SLOTS[j] = (first, len(SLOT) - first)
NSLOT = len(SLOT)
PACK = 112

YSTEPS = ((4, -3), (3, -2), (2, -1), (1,))
YHEADS = (4, -3)
YSLOT = {("f", 3): 0, ("f", 2): 1, ("f", 1): 2, ("f", 0): 3, ("b", -2): 4, ("b", -1): 5, ("b", 0): 6}

SUMS, WX, WD, PG = 0, 1, 3, 5
DD = 6
ZC = DD + len(GROUPS)
YC = ZC + len(JOINS)
YF = YC + 7 * S
NRECV = YF + 1
S_SUMS, S_WX, S_WD, S_PG, S_DD, S_Z, S_Y, S_YF = range(8)
L_QG, L_GAIN, L_WH, L_OUT = 2 * KC, 2 * KC + 1, 2 * KC + 2, 2 * KC + 3


def dot(a, b, dims):
    return lax.dot_general(a, b, (dims, ((), ())), preferred_element_type=F32)


def packed(v):
    rest = v[:, 128:]
    tile = rest[:16]
    for j in (1, 2, 3):
        tile = tile + pltpu.roll(rest[16 * j : 16 * j + 16], 32 * j, 1)
    return v[:, :128], tile, rest[64:]


def kernel(
    x_hbm, w_hbm, gain_hbm, qg_hbm, ig_hbm, wg_hbm,
    x_v, xt_v, w_v, wst_v, gain_v, qg_v, sums_v, pga_v, pgs_v, pgt_v,
    dsend, drecv, own_v, zx_v, zs_v, zrecv, wg_v,
    part_v, ysend, yrecv, yfin, out_v,
    lsem, ssem, rsem,
):
    d = lax.axis_index("dp")
    t = lax.axis_index("tensor")
    core = lax.rem(d, 2)
    z = lax.rem(lax.div(d, 2), NZ)
    xh = lax.div(d, 2 * NZ)
    y = lax.rem(t, NY)
    xl = lax.div(t, NY)
    sgn = 1 - 2 * core

    def dev(xh_, z_, core_, xl_, y_):
        return {"dp": (xh_ * NZ + z_) * 2 + core_, "tensor": xl_ * NY + y_}

    def zat(r):
        return lax.rem(z + sgn * r + 2 * NZ, NZ)

    def yat(r):
        return lax.rem(y + sgn * r + 2 * NY, NY)

    sibling = dev(xh, z, 1 - core, xl, y)
    partner = dev(xh, z, core, 1 - xl, y)
    across = dev(1 - xh, z, core, 1 - xl, y)

    loads = []
    for k in range(KC):
        cols = pl.ds(k * KW, KW)
        loads.append((
            pltpu.make_async_copy(x_hbm.at[:, cols], x_v.at[:, cols], lsem.at[k]),
            pltpu.make_async_copy(w_hbm.at[:, cols], w_v.at[:, cols], lsem.at[KC + k]),
        ))
    for a, b in loads:
        a.start()
        b.start()
    qg_load = pltpu.make_async_copy(qg_hbm, qg_v, lsem.at[L_QG])
    qg_load.start()
    gain_load = pltpu.make_async_copy(gain_hbm, gain_v, lsem.at[L_GAIN])
    gain_load.start()
    myhalf = pl.ds(pl.multiple_of(xl * HALF, 128), HALF)
    otherhalf = pl.ds(pl.multiple_of((1 - xl) * HALF, 128), HALF)
    wh_load = pltpu.make_async_copy(w_hbm.at[:, myhalf], wst_v.at[:F], lsem.at[L_WH])
    wh_load.start()

    barrier = pltpu.get_barrier_semaphore()
    peers = [{"dp": d, "tensor": lax.rem(t + o, NT)} for o in range(1, NT)]
    peers += [across, sibling]
    peers += [dev(xh, zat(r), core, xl, y) for r in (1, -1, 2, -2, 5, -5)]
    peers += [dev(1 - xh, zat(r), core, xl, y) for r in (0, 1, -1, 2, -2)]
    for p in peers:
        pl.semaphore_signal(barrier, inc=1, device_id=p, device_id_type=MESH)

    pt = None
    for k, (a, b) in enumerate(loads):
        a.wait()
        b.wait()
        cols = slice(k * KW, (k + 1) * KW)
        term = dot(w_v[:, cols], x_v[:, cols], ((1,), (1,)))
        pt = term if pt is None else pt + term
    qg_load.wait()
    gain_load.wait()
    rows = lax.broadcasted_iota(jnp.int32, (F, F), 0)
    lanes = lax.broadcasted_iota(jnp.int32, (F, F), 1)
    gain = jnp.sum(jnp.where(rows == lanes, gain_v[...], 0.0), axis=1, keepdims=True)
    sg = qg_v[...].astype(F32) * gain
    sq = jnp.sum(pt * pt, axis=0, keepdims=True)
    cr = jnp.sum(sg * pt, axis=0, keepdims=True)
    sums_v[t, 0:1, :] = sq[:, :128]
    sums_v[t, 1:2, :] = sq[:, 128:]
    sums_v[t, 2:3, :] = cr[:, :128]
    sums_v[t, 3:4, :] = cr[:, 128:]

    pl.semaphore_wait(barrier, len(peers))

    def send(src, dst, ssem_at, rsem_at, device):
        pltpu.make_async_remote_copy(
            src_ref=src, dst_ref=dst, send_sem=ssem.at[ssem_at], recv_sem=rsem.at[rsem_at],
            device_id=device, device_id_type=MESH,
        ).start()

    def handle(ref, ssem_at, rsem_at):
        return pltpu.make_async_remote_copy(
            src_ref=ref, dst_ref=ref, send_sem=ssem.at[ssem_at], recv_sem=rsem.at[rsem_at],
            device_id=sibling, device_id_type=MESH,
        )

    def arrived(ref, rsem_at):
        handle(ref, 0, rsem_at).wait_recv()

    def left(ref, ssem_at):
        handle(ref, ssem_at, 0).wait_send()

    for p in peers[: NT - 1]:
        send(sums_v.at[t], sums_v.at[t], S_SUMS, SUMS, p)

    wpart = wst_v.at[F:]
    for n, who in enumerate((partner, across)):
        src = pl.ds(pl.multiple_of((1 - xl) * HALF + (2 * n + core) * CS, 128), CS)
        dst = pl.ds(pl.multiple_of((2 * n + core) * CS, 128), CS)
        send(w_v.at[:, src], wpart.at[:, dst], S_WX, WX + n, who)

    for k in range(D // 256):
        turned = x_v[:, k * 256 : (k + 1) * 256].T
        at, end = k * 256, (k + 1) * 256
        while at < end:
            h, zz, o = at // HALF, at % HALF // 160, at % 160
            n = min(160 - o, end - at)
            xt_v[zz, h * 160 + o : h * 160 + o + n, :] = turned[at - k * 256 : at - k * 256 + n]
            at += n
    pga_v[F:, :] = jnp.zeros((256 - F, T), BF16)

    arrived(sums_v.at[: NT - 1], SUMS)
    total = sums_v[0]
    for s in range(1, NT):
        total = total + sums_v[s]
    sq = jnp.concatenate([total[0:1], total[1:2]], axis=1)
    cr = jnp.concatenate([total[2:3], total[3:4]], axis=1)
    inv = 1.0 / jnp.sqrt(sq / HQ + epsilon)
    coef = inv * inv * inv * (cr / HQ)
    pg = (inv * sg - coef * pt).astype(BF16)
    pga_v[:F, :] = pg
    pgs_v[:F, :] = pg
    send(pga_v.at[:F], pgs_v.at[F:], S_PG, PG, partner)

    def blocks(g):
        for r in GROUPS[g]:
            v = dot(xt_v[zat(r)], pga_v[...], ((1,), (1,)))
            mirror = r if r in (0, 8) else -r
            for h in (0, 1):
                a, b = v[h * 160 : h * 160 + 80], v[h * 160 + 80 : h * 160 + 160]
                mine = packed(jnp.where(core == 0, a, b))
                other = packed(jnp.where(core == 0, b, a))
                for ref, i, parts in ((own_v, AT[r], mine), (dsend, AT[mirror], other)):
                    ref[i, h, :80, :] = parts[0].astype(ref.dtype)
                    ref[i, h, 80:96, :] = parts[1].astype(ref.dtype)
                    ref[i, h, 96:, :] = parts[2].astype(ref.dtype)
        at = pl.ds(AT[GROUPS[g][0]], len(GROUPS[g]))
        send(dsend.at[at], drecv.at[at], S_DD, DD + g, sibling)

    def local(r, h):
        return own_v[AT[r], h] + drecv[AT[r], h].astype(F32)

    def zsend(r, v):
        i, slot = AT[r], SLOT["own", r]
        zs_v[i] = v.astype(BF16)
        send(
            zs_v.at[i], zrecv.at[slot], S_Z, ZC + JOINS.index(PARENT[r]),
            dev(xh, zat(r - PARENT[r]), core, xl, y),
        )

    def zleaf(g):
        at = pl.ds(AT[GROUPS[g][0]], len(GROUPS[g]))
        arrived(drecv.at[at], DD + g)
        for r in GROUPS[g]:
            i, slot = AT[r], SLOT["cross", r]
            zx_v[i] = local(r, 1 - xh).astype(BF16)
            send(
                zx_v.at[i], zrecv.at[slot], S_Z, ZC + JOINS.index(CROSS[r]),
                dev(1 - xh, zat(r - CROSS[r]), core, xl, y),
            )
            if r not in JOINS:
                zsend(r, local(r, xh))

    def joined(r):
        first, n = JOIN_SLOTS[r]
        arrived(zrecv.at[pl.ds(first, n)], ZC + JOINS.index(r))
        v = local(r, xh)
        for k in range(first, first + n):
            v = v + zrecv[k].astype(F32)
        return v

    def zstage(k):
        for r in STAGES[k]:
            zsend(r, joined(r))

    def yrows(r):
        return pl.multiple_of(yat(r) * 16, 16)

    def ystep(k, s):
        for r in YSTEPS[k]:
            side, nxt = ("f", r - 1) if r > 0 else ("b", r + 1)
            at = yrows(r)
            new = [part_v[s, pl.ds(at + h * 128, 16), :] for h in (0, 1)]
            if r not in YHEADS:
                slot = YSLOT[side, r]
                arrived(yrecv.at[slot, s], YC + slot * S + s)
                new = [v + yrecv[slot, s, h * 16 : h * 16 + 16, :].astype(F32) for h, v in enumerate(new)]
            slot = YSLOT[side, nxt]
            for h, v in enumerate(new):
                ysend[slot, s, h * 16 : h * 16 + 16, :] = v.astype(BF16)
            send(
                ysend.at[slot, s], yrecv.at[slot, s], S_Y, YC + slot * S + s,
                dev(xh, z, core, xl, yat(1 if r > 0 else -1)),
            )

    blocks(0)
    blocks(1)
    zleaf(0)
    blocks(2)
    zleaf(1)
    blocks(3)
    zleaf(2)
    zleaf(3)

    for n in (0, 1):
        cols = pl.ds(pl.multiple_of((2 * n + core) * CS, 128), CS)
        arrived(wpart.at[:, cols], WX + n)
        send(wpart.at[:, cols], wpart.at[:, cols], S_WD, WD + n, sibling)
    wh_load.wait()
    arrived(pgs_v.at[F:], PG)
    pgt_v[...] = pgs_v[...].T
    for n in (0, 1):
        cols = pl.ds(pl.multiple_of((2 * n + 1 - core) * CS, 128), CS)
        arrived(wpart.at[:, cols], WD + n)
    for s in range(S):
        part_v[s] = dot(pgt_v[...], wst_v[:, s * CS : (s + 1) * CS], ((1,), (0,)))
        ystep(0, s)

    zstage(0)
    for s in range(S):
        ystep(1, s)
    zstage(1)
    for s in range(S):
        ystep(2, s)
    for s in range(S):
        ystep(3, s)

    for s in range(S):
        slots = (YSLOT["f", 0], YSLOT["b", 0])
        for slot in slots:
            arrived(yrecv.at[slot, s], YC + slot * S + s)
        for h in (0, 1):
            rows = slice(h * 16, h * 16 + 16)
            v = part_v[s, pl.ds(yrows(0) + h * 128, 16), :]
            for slot in slots:
                v = v + yrecv[slot, s, rows, :].astype(F32)
            yfin[s, rows, :] = v.astype(BF16)
        cols = pl.ds(pl.multiple_of(xl * HALF + s * CS, 128), CS)
        send(yfin.at[s, pl.ds(pl.multiple_of((1 - xl) * 16, 16), 16)], out_v.at[:, cols], S_YF, YF, partner)
        out_v[:, cols] = yfin[s, pl.ds(pl.multiple_of(xl * 16, 16), 16), :]
    outs = [pltpu.make_async_copy(out_v.at[:, myhalf], ig_hbm.at[:, myhalf], lsem.at[L_OUT])]
    outs[0].start()

    v = joined(0)
    wg_v[:, :128] = v[:80]
    wg_v[:16, 128:] = v[80:96, :32]
    for j in (1, 2, 3):
        wg_v[16 * j : 16 * j + 16, 128:] = pltpu.roll(v[80:96], 128 - 32 * j, 1)[:, :32]
    wg_v[64:, 128:] = v[96:, :32]
    outs.append(pltpu.make_async_copy(wg_v, wg_hbm, lsem.at[L_OUT + 1]))
    outs[1].start()

    arrived(out_v.at[:, otherhalf], YF)
    outs.append(pltpu.make_async_copy(out_v.at[:, otherhalf], ig_hbm.at[:, otherhalf], lsem.at[L_OUT + 2]))
    outs[2].start()
    left(sums_v.at[: NT - 1], S_SUMS)
    left(wpart.at[:, : 2 * CS], S_WX)
    left(wpart.at[:, : 2 * CS], S_WD)
    left(pgs_v.at[F:], S_PG)
    left(dsend, S_DD)
    left(zrecv, S_Z)
    left(yrecv, S_Y)
    left(out_v.at[:, otherhalf], S_YF)
    for copy in outs:
        copy.wait()


def per_device(block_input, query_weight, query_gain, query_grad):
    hbm = pl.BlockSpec(memory_space=pltpu.HBM)
    anywhere = pl.BlockSpec(memory_space=pl.ANY)
    return pl.pallas_call(
        kernel,
        out_shape=(
            jax.ShapeDtypeStruct((T // NT, D), BF16),
            jax.ShapeDtypeStruct((80, F), F32),
        ),
        in_specs=[hbm, hbm, hbm, hbm],
        out_specs=(anywhere, anywhere),
        scratch_shapes=[
            pltpu.VMEM((T, D), BF16),
            pltpu.VMEM((NZ, 320, T), BF16),
            pltpu.VMEM((F, D), BF16),
            pltpu.VMEM((2 * F, HALF), BF16),
            pltpu.VMEM((1, F), F32),
            pltpu.VMEM((F, T), BF16),
            pltpu.VMEM((NT, 4, 128), F32),
            pltpu.VMEM((256, T), BF16),
            pltpu.VMEM((2 * F, T), BF16),
            pltpu.VMEM((T, 2 * F), BF16),
            pltpu.VMEM((16, 2, PACK, 128), BF16),
            pltpu.VMEM((16, 2, PACK, 128), BF16),
            pltpu.VMEM((16, 2, PACK, 128), F32),
            pltpu.VMEM((16, PACK, 128), BF16),
            pltpu.VMEM((16, PACK, 128), BF16),
            pltpu.VMEM((NSLOT, PACK, 128), BF16),
            pltpu.VMEM((80, F), F32),
            pltpu.VMEM((S, T, CS), F32),
            pltpu.VMEM((7, S, 32, CS), BF16),
            pltpu.VMEM((7, S, 32, CS), BF16),
            pltpu.VMEM((S, 32, CS), BF16),
            pltpu.VMEM((T // NT, D), BF16),
            pltpu.SemaphoreType.DMA((L_OUT + 3,)),
            pltpu.SemaphoreType.DMA((8,)),
            pltpu.SemaphoreType.DMA((NRECV,)),
        ],
        compiler_params=pltpu.CompilerParams(
            collective_id=0, has_side_effects=True, vmem_limit_bytes=40 * 1024 * 1024
        ),
    )(*(pltpu.with_memory_space_constraint(a, pltpu.HBM) for a in (block_input, query_weight, query_gain.reshape(1, F), query_grad)))


def solution(mesh):
    return jax.shard_map(
        per_device,
        mesh=mesh,
        in_specs=(P("dp", None), P("tensor", None), P("tensor"), P("tensor", "dp")),
        out_specs=(P(("dp", "tensor"), None), P("dp", "tensor")),
        check_vma=False,
    )
```

```python
import jax
import jax.numpy as jnp
from jax import lax
from jax.experimental import pallas as pl
from jax.experimental.pallas import tpu as pltpu
from jax.sharding import PartitionSpec as P

MESH = pl.DeviceIdType.MESH
F32, BF16 = jnp.float32, jnp.bfloat16

NT, NY, NZ = 16, 8, 16
T, F, D = 256, 160, 5120
HALF = D // 2
S = 4
CS = HALF // S
KC = 4
KW = D // KC
HQ = F * NT
epsilon = 1e-6

PARENT = {8: 7, 7: 5, 6: 5, 5: 0, 4: 3, 3: 1, 2: 1, 1: 0, -7: -5, -6: -5, -5: 0, -4: -3, -3: -1, -2: -1, -1: 0}
CROSS = {8: 7, 7: 7, 6: 5, 5: 5, -7: -5, -6: -5, -5: -5, 1: 0, -1: 0, 0: 0}
GROUPS = ((8, 7, -7), (6, -6, 5, -5), (4, -4, 3, -3), (2, -2, 1, -1, 0))
ORDER = sum(GROUPS, ())
AT = {r: i for i, r in enumerate(ORDER)}
JOINS = (7, 5, -5, 3, -3, 1, -1, 0)
SLOT, JOIN_SLOTS = {}, {}
count = 0
for j in JOINS:
    first = count
    for r in ORDER:
        if PARENT.get(r) == j:
            SLOT["own", r] = count
            count += 2 if abs(r) < 5 and j else 1
        if CROSS.get(r) == j:
            SLOT["cross", r] = count
            count += 1
    JOIN_SLOTS[j] = (first, count - first)
NSLOT = count
PACK = 112

YSTEPS = ((4, -3), (3, -2), (2, -1), (1,))
YHEADS = (4, -3)
YSLOT = {("f", 3): 0, ("f", 2): 1, ("f", 1): 2, ("f", 0): 3, ("b", -2): 4, ("b", -1): 5, ("b", 0): 6}

SUMS, WX, WD, PG = 0, 1, 3, 5
DD = 6
ZC = DD + len(GROUPS)
YC = ZC + len(JOINS)
YF = YC + 7 * S
NRECV = YF + 1
S_SUMS, S_WX, S_WD, S_PG, S_DD, S_Z, S_Y, S_YF = range(8)
L_QG, L_GAIN, L_WH, L_OUT = 2 * KC, 2 * KC + 1, 2 * KC + 2, 2 * KC + 3


def dot(a, b, dims):
    return lax.dot_general(a, b, (dims, ((), ())), preferred_element_type=F32)


def packed(v):
    rest = v[:, 128:]
    tile = rest[:16]
    for j in (1, 2, 3):
        tile = tile + pltpu.roll(rest[16 * j : 16 * j + 16], 32 * j, 1)
    return v[:, :128], tile, rest[64:]


def kernel(
    x_hbm, w_hbm, gain_hbm, qg_hbm, ig_hbm, wg_hbm,
    x_v, xt_v, w_v, wst_v, gain_v, qg_v, sums_v, pga_v, pgp_v, sgt_v, ptt_v,
    dsend, drecv, own_v, zs_v, zrecv, wg_v,
    part_v, ysend, yrecv, yfin, out_v,
    lsem, ssem, rsem,
):
    d = lax.axis_index("dp")
    t = lax.axis_index("tensor")
    core = lax.rem(d, 2)
    z = lax.rem(lax.div(d, 2), NZ)
    xh = lax.div(d, 2 * NZ)
    y = lax.rem(t, NY)
    xl = lax.div(t, NY)
    sgn = 1 - 2 * core

    def dev(xh_, z_, core_, xl_, y_):
        return {"dp": (xh_ * NZ + z_) * 2 + core_, "tensor": xl_ * NY + y_}

    def zat(r):
        return lax.rem(z + sgn * r + 2 * NZ, NZ)

    def yat(r):
        return lax.rem(y + sgn * r + 2 * NY, NY)

    sibling = dev(xh, z, 1 - core, xl, y)
    partner = dev(xh, z, core, 1 - xl, y)
    across = dev(1 - xh, z, core, 1 - xl, y)

    loads = []
    for k in range(KC):
        cols = pl.ds(k * KW, KW)
        loads.append((
            pltpu.make_async_copy(x_hbm.at[:, cols], x_v.at[:, cols], lsem.at[k]),
            pltpu.make_async_copy(w_hbm.at[:, cols], w_v.at[:, cols], lsem.at[KC + k]),
        ))
    for a, b in loads:
        a.start()
        b.start()
    qg_load = pltpu.make_async_copy(qg_hbm, qg_v, lsem.at[L_QG])
    qg_load.start()
    gain_load = pltpu.make_async_copy(gain_hbm, gain_v, lsem.at[L_GAIN])
    gain_load.start()
    myhalf = pl.ds(pl.multiple_of(xl * HALF, 128), HALF)
    otherhalf = pl.ds(pl.multiple_of((1 - xl) * HALF, 128), HALF)
    wh_load = pltpu.make_async_copy(w_hbm.at[:, myhalf], wst_v.at[:F], lsem.at[L_WH])
    wh_load.start()

    barrier = pltpu.get_barrier_semaphore()
    peers = [{"dp": d, "tensor": lax.rem(t + o, NT)} for o in range(1, NT)]
    peers += [across, sibling]
    peers += [dev(xh, zat(r), core, xl, y) for r in (1, -1, 2, -2, 5, -5)]
    peers += [dev(1 - xh, zat(r), core, xl, y) for r in (0, 1, -1, 2, -2)]
    for p in peers:
        pl.semaphore_signal(barrier, inc=1, device_id=p, device_id_type=MESH)

    pt = None
    for k, (a, b) in enumerate(loads):
        a.wait()
        b.wait()
        cols = slice(k * KW, (k + 1) * KW)
        term = dot(w_v[:, cols], x_v[:, cols], ((1,), (1,)))
        pt = term if pt is None else pt + term
    qg_load.wait()
    gain_load.wait()
    rows = lax.broadcasted_iota(jnp.int32, (F, F), 0)
    lanes = lax.broadcasted_iota(jnp.int32, (F, F), 1)
    gain = jnp.sum(jnp.where(rows == lanes, gain_v[...], 0.0), axis=1, keepdims=True)
    sg = qg_v[...].astype(F32) * gain
    sq = jnp.sum(pt * pt, axis=0, keepdims=True)
    cr = jnp.sum(sg * pt, axis=0, keepdims=True)
    sums_v[t, 0:1, :] = sq[:, :128]
    sums_v[t, 1:2, :] = sq[:, 128:]
    sums_v[t, 2:3, :] = cr[:, :128]
    sums_v[t, 3:4, :] = cr[:, 128:]

    pl.semaphore_wait(barrier, len(peers))

    def send(src, dst, ssem_at, rsem_at, device):
        pltpu.make_async_remote_copy(
            src_ref=src, dst_ref=dst, send_sem=ssem.at[ssem_at], recv_sem=rsem.at[rsem_at],
            device_id=device, device_id_type=MESH,
        ).start()

    def handle(ref, ssem_at, rsem_at):
        return pltpu.make_async_remote_copy(
            src_ref=ref, dst_ref=ref, send_sem=ssem.at[ssem_at], recv_sem=rsem.at[rsem_at],
            device_id=sibling, device_id_type=MESH,
        )

    def arrived(ref, rsem_at):
        handle(ref, 0, rsem_at).wait_recv()

    def left(ref, ssem_at):
        handle(ref, ssem_at, 0).wait_send()

    for p in peers[: NT - 1]:
        send(sums_v.at[t], sums_v.at[t], S_SUMS, SUMS, p)

    wpart = wst_v.at[F:]
    for n, who in enumerate((partner, across)):
        src = pl.ds(pl.multiple_of((1 - xl) * HALF + (2 * n + core) * CS, 128), CS)
        dst = pl.ds(pl.multiple_of((2 * n + core) * CS, 128), CS)
        send(w_v.at[:, src], wpart.at[:, dst], S_WX, WX + n, who)

    for k in range(D // 256):
        turned = x_v[:, k * 256 : (k + 1) * 256].T
        at, end = k * 256, (k + 1) * 256
        while at < end:
            h, zz, o = at // HALF, at % HALF // 160, at % 160
            n = min(160 - o, end - at)
            xt_v[zz, h * 160 + o : h * 160 + o + n, :] = turned[at - k * 256 : at - k * 256 + n]
            at += n
    pga_v[F:, :] = jnp.zeros((256 - F, T), BF16)
    sgt_v[...] = sg.T
    ptt_v[...] = pt.T

    arrived(sums_v.at[: NT - 1], SUMS)
    total = sums_v[0]
    for s in range(1, NT):
        total = total + sums_v[s]
    sq = jnp.concatenate([total[0:1], total[1:2]], axis=1)
    cr = jnp.concatenate([total[2:3], total[3:4]], axis=1)
    inv = 1.0 / jnp.sqrt(sq / HQ + epsilon)
    coef = inv * inv * inv * (cr / HQ)
    pg = (inv * sg - coef * pt).astype(BF16)
    pga_v[:F, :] = pg
    send(pga_v.at[:F], pgp_v, S_PG, PG, partner)

    def blocks(g):
        for r in GROUPS[g]:
            v = dot(xt_v[zat(r)], pga_v[...], ((1,), (1,)))
            mirror = r if r in (0, 8) else -r
            for h in (0, 1):
                a, b = v[h * 160 : h * 160 + 80], v[h * 160 + 80 : h * 160 + 160]
                mine = packed(jnp.where(core == 0, a, b))
                other = packed(jnp.where(core == 0, b, a))
                for ref, i, parts in ((own_v, AT[r], mine), (dsend, AT[mirror], other)):
                    ref[i, h, :80, :] = parts[0].astype(ref.dtype)
                    ref[i, h, 80:96, :] = parts[1].astype(ref.dtype)
                    ref[i, h, 96:, :] = parts[2].astype(ref.dtype)
        at = pl.ds(AT[GROUPS[g][0]], len(GROUPS[g]))
        send(dsend.at[at], drecv.at[at], S_DD, DD + g, sibling)

    def local(r, h):
        return own_v[AT[r], h] + drecv[AT[r], h].astype(F32)

    def zcross(r, v):
        zs_v[AT[r], 1 - xh] = v.astype(BF16)
        send(
            zs_v.at[AT[r], 1 - xh], zrecv.at[SLOT["cross", r]], S_Z, ZC + JOINS.index(CROSS[r]),
            dev(1 - xh, zat(r - CROSS[r]), core, xl, y),
        )

    def zown(r, v):
        zs_v[AT[r], xh] = v.astype(BF16)
        send(
            zs_v.at[AT[r], xh], zrecv.at[SLOT["own", r]], S_Z, ZC + JOINS.index(PARENT[r]),
            dev(xh, zat(r - PARENT[r]), core, xl, y),
        )

    def zboth(r, pair):
        for h, v in enumerate(pair):
            zs_v[AT[r], h] = v.astype(BF16)
        send(
            zs_v.at[AT[r]], zrecv.at[pl.ds(SLOT["own", r], 2)], S_Z, ZC + JOINS.index(PARENT[r]),
            dev(xh, zat(r - PARENT[r]), core, xl, y),
        )

    def zleaf(g):
        at = pl.ds(AT[GROUPS[g][0]], len(GROUPS[g]))
        arrived(drecv.at[at], DD + g)
        for r in GROUPS[g]:
            if abs(r) >= 5 or r == 0:
                zcross(r, local(r, 1 - xh))
            if r not in JOINS:
                if abs(r) >= 5:
                    zown(r, local(r, xh))
                else:
                    zboth(r, [local(r, h) for h in (0, 1)])

    def joined(r):
        first, n = JOIN_SLOTS[r]
        arrived(zrecv.at[pl.ds(first, n)], ZC + JOINS.index(r))
        slots = range(first, first + n)
        if abs(r) >= 5 or r == 0:
            v = local(r, xh)
            for k in slots:
                v = v + zrecv[k].astype(F32)
            return v
        pair = []
        for h in ((0, 1) if abs(r) == 3 else (xh, 1 - xh)):
            v = local(r, h)
            for k in range(first, first + n, 2):
                v = v + zrecv[k + h].astype(F32)
            pair.append(v)
        return pair

    def zjoin(r):
        v = joined(r)
        if abs(r) == 5 or r == 7:
            zown(r, v)
        elif abs(r) == 3:
            zboth(r, v)
        else:
            zcross(r, v[1])
            zown(r, v[0])

    def yrows(r):
        return pl.multiple_of(yat(r) * 16, 16)

    def ystep(k, s):
        for r in YSTEPS[k]:
            side, nxt = ("f", r - 1) if r > 0 else ("b", r + 1)
            at = yrows(r)
            new = [part_v[s, pl.ds(at + h * 128, 16), :] for h in (0, 1)]
            if r not in YHEADS:
                slot = YSLOT[side, r]
                arrived(yrecv.at[slot, s], YC + slot * S + s)
                new = [v + yrecv[slot, s, h * 16 : h * 16 + 16, :].astype(F32) for h, v in enumerate(new)]
            slot = YSLOT[side, nxt]
            for h, v in enumerate(new):
                ysend[slot, s, h * 16 : h * 16 + 16, :] = v.astype(BF16)
            send(
                ysend.at[slot, s], yrecv.at[slot, s], S_Y, YC + slot * S + s,
                dev(xh, z, core, xl, yat(1 if r > 0 else -1)),
            )

    blocks(0)
    blocks(1)
    for n in (0, 1):
        cols = pl.ds(pl.multiple_of((2 * n + core) * CS, 128), CS)
        arrived(wpart.at[:, cols], WX + n)
        send(wpart.at[:, cols], wpart.at[:, cols], S_WD, WD + n, sibling)
    wh_load.wait()
    both = jnp.concatenate([inv, coef], axis=0)
    both = jnp.concatenate([both, jnp.zeros((6, T), F32)], axis=0).T
    own = (both[:, 0:1] * sgt_v[...] - both[:, 1:2] * ptt_v[...]).astype(BF16)
    for s in range(S):
        part_v[s] = dot(own, wst_v[:F, s * CS : (s + 1) * CS], ((1,), (0,)))
    zleaf(0)
    arrived(pgp_v, PG)
    theirs = pgp_v[...].T
    for n in (0, 1):
        cols = pl.ds(pl.multiple_of((2 * n + 1 - core) * CS, 128), CS)
        arrived(wpart.at[:, cols], WD + n)
    for s in range(S):
        part_v[s] += dot(theirs, wst_v[F:, s * CS : (s + 1) * CS], ((1,), (0,)))
        ystep(0, s)
    blocks(2)
    zleaf(1)
    blocks(3)
    zleaf(2)
    zleaf(3)
    zjoin(7)
    zjoin(-5)
    for s in range(S):
        ystep(1, s)
    zjoin(3)
    zjoin(-3)
    zjoin(5)
    for s in range(S):
        ystep(2, s)
    zjoin(1)
    zjoin(-1)
    for s in range(S):
        ystep(3, s)

    for s in range(S):
        slots = (YSLOT["f", 0], YSLOT["b", 0])
        for slot in slots:
            arrived(yrecv.at[slot, s], YC + slot * S + s)
        for h in (0, 1):
            rows = slice(h * 16, h * 16 + 16)
            v = part_v[s, pl.ds(yrows(0) + h * 128, 16), :]
            for slot in slots:
                v = v + yrecv[slot, s, rows, :].astype(F32)
            yfin[s, rows, :] = v.astype(BF16)
        cols = pl.ds(pl.multiple_of(xl * HALF + s * CS, 128), CS)
        send(yfin.at[s, pl.ds(pl.multiple_of((1 - xl) * 16, 16), 16)], out_v.at[:, cols], S_YF, YF, partner)
        out_v[:, cols] = yfin[s, pl.ds(pl.multiple_of(xl * 16, 16), 16), :]
    outs = [pltpu.make_async_copy(out_v.at[:, myhalf], ig_hbm.at[:, myhalf], lsem.at[L_OUT])]
    outs[0].start()

    v = joined(0)
    wg_v[:, :128] = v[:80]
    wg_v[:16, 128:] = v[80:96, :32]
    for j in (1, 2, 3):
        wg_v[16 * j : 16 * j + 16, 128:] = pltpu.roll(v[80:96], 128 - 32 * j, 1)[:, :32]
    wg_v[64:, 128:] = v[96:, :32]
    outs.append(pltpu.make_async_copy(wg_v, wg_hbm, lsem.at[L_OUT + 1]))
    outs[1].start()

    arrived(out_v.at[:, otherhalf], YF)
    outs.append(pltpu.make_async_copy(out_v.at[:, otherhalf], ig_hbm.at[:, otherhalf], lsem.at[L_OUT + 2]))
    outs[2].start()
    left(sums_v.at[: NT - 1], S_SUMS)
    left(wpart.at[:, : 2 * CS], S_WX)
    left(wpart.at[:, : 2 * CS], S_WD)
    left(pgp_v, S_PG)
    left(dsend, S_DD)
    left(zrecv, S_Z)
    left(yrecv, S_Y)
    left(out_v.at[:, otherhalf], S_YF)
    for copy in outs:
        copy.wait()


def per_device(block_input, query_weight, query_gain, query_grad):
    hbm = pl.BlockSpec(memory_space=pltpu.HBM)
    anywhere = pl.BlockSpec(memory_space=pl.ANY)
    return pl.pallas_call(
        kernel,
        out_shape=(
            jax.ShapeDtypeStruct((T // NT, D), BF16),
            jax.ShapeDtypeStruct((80, F), F32),
        ),
        in_specs=[hbm, hbm, hbm, hbm],
        out_specs=(anywhere, anywhere),
        scratch_shapes=[
            pltpu.VMEM((T, D), BF16),
            pltpu.VMEM((NZ, 320, T), BF16),
            pltpu.VMEM((F, D), BF16),
            pltpu.VMEM((2 * F, HALF), BF16),
            pltpu.VMEM((1, F), F32),
            pltpu.VMEM((F, T), BF16),
            pltpu.VMEM((NT, 4, 128), F32),
            pltpu.VMEM((256, T), BF16),
            pltpu.VMEM((F, T), BF16),
            pltpu.VMEM((T, F), F32),
            pltpu.VMEM((T, F), F32),
            pltpu.VMEM((16, 2, PACK, 128), BF16),
            pltpu.VMEM((16, 2, PACK, 128), BF16),
            pltpu.VMEM((16, 2, PACK, 128), F32),
            pltpu.VMEM((16, 2, PACK, 128), BF16),
            pltpu.VMEM((NSLOT, PACK, 128), BF16),
            pltpu.VMEM((80, F), F32),
            pltpu.VMEM((S, T, CS), F32),
            pltpu.VMEM((7, S, 32, CS), BF16),
            pltpu.VMEM((7, S, 32, CS), BF16),
            pltpu.VMEM((S, 32, CS), BF16),
            pltpu.VMEM((T // NT, D), BF16),
            pltpu.SemaphoreType.DMA((L_OUT + 3,)),
            pltpu.SemaphoreType.DMA((8,)),
            pltpu.SemaphoreType.DMA((NRECV,)),
        ],
        compiler_params=pltpu.CompilerParams(
            collective_id=0, has_side_effects=True, vmem_limit_bytes=40 * 1024 * 1024
        ),
    )(*(pltpu.with_memory_space_constraint(a, pltpu.HBM) for a in (block_input, query_weight, query_gain.reshape(1, F), query_grad)))


def solution(mesh):
    return jax.shard_map(
        per_device,
        mesh=mesh,
        in_specs=(P("dp", None), P("tensor", None), P("tensor"), P("tensor", "dp")),
        out_specs=(P(("dp", "tensor"), None), P("dp", "tensor")),
        check_vma=False,
    )
```

```python
import jax
import jax.numpy as jnp
from jax import lax
from jax.experimental import pallas as pl
from jax.experimental.pallas import tpu as pltpu
from jax.sharding import PartitionSpec as P

MESH = pl.DeviceIdType.MESH
F32, BF16 = jnp.float32, jnp.bfloat16

NT, NY, NZ = 16, 8, 16
T, F, D = 256, 160, 5120
HALF = D // 2
S = 4
CS = HALF // S
KC = 4
KW = D // KC
HQ = F * NT
epsilon = 1e-6

PARENT = {8: 7, 7: 5, 6: 5, 5: 0, 4: 3, 3: 1, 2: 1, 1: 0, -7: -5, -6: -5, -5: 0, -4: -3, -3: -1, -2: -1, -1: 0}
CROSS = {8: 7, 7: 7, 6: 5, 5: 5, -7: -5, -6: -5, -5: -5, 1: 0, -1: 0, 0: 0}
GROUPS = ((8, 7, -7), (6, -6, 5, -5), (4, -4, 3, -3), (2, -2, 1, -1, 0))
ORDER = sum(GROUPS, ())
AT = {r: i for i, r in enumerate(ORDER)}
JOINS = (7, 5, -5, 3, -3, 1, -1, 0)
SLOT, JOIN_SLOTS = {}, {}
count = 0
for j in JOINS:
    first = count
    for r in ORDER:
        if PARENT.get(r) == j:
            SLOT["own", r] = count
            count += 2 if abs(r) < 5 and j else 1
        if CROSS.get(r) == j:
            SLOT["cross", r] = count
            count += 1
    JOIN_SLOTS[j] = (first, count - first)
NSLOT = count
PACK = 112

YSTEPS = ((4, -3), (3, -2), (2, -1), (1,))
YHEADS = (4, -3)
YSLOT = {3: 0, 2: 1, 1: 2, -2: 3, -1: 4}

SUMS, WX, WD, PG = 0, 1, 3, 5
DD = 6
ZC = DD + len(GROUPS)
YC = ZC + len(JOINS)
YF = YC + 5 * S
NRECV = YF + S
S_SUMS, S_WX, S_WD, S_PG, S_DD, S_Z, S_Y, S_YF = range(8)
L_QG, L_GAIN, L_WH, L_OUT = 2 * KC, 2 * KC + 1, 2 * KC + 2, 2 * KC + 3


def dot(a, b, dims):
    return lax.dot_general(a, b, (dims, ((), ())), preferred_element_type=F32)


def packed(v):
    rest = v[:, 128:]
    tile = rest[:16]
    for j in (1, 2, 3):
        tile = tile + pltpu.roll(rest[16 * j : 16 * j + 16], 32 * j, 1)
    return v[:, :128], tile, rest[64:]


def kernel(
    x_hbm, w_hbm, gain_hbm, qg_hbm, ig_hbm, wg_hbm,
    x_v, xt_v, w_v, wst_v, gain_v, qg_v, sums_v, pga_v, pgp_v, sgt_v, ptt_v,
    dsend, drecv, own_v, zs_v, zrecv, wg_v,
    part_v, ysend, yrecv, ylast, yfin, out_v,
    lsem, ssem, rsem,
):
    d = lax.axis_index("dp")
    t = lax.axis_index("tensor")
    core = lax.rem(d, 2)
    z = lax.rem(lax.div(d, 2), NZ)
    xh = lax.div(d, 2 * NZ)
    y = lax.rem(t, NY)
    xl = lax.div(t, NY)
    sgn = 1 - 2 * core

    def dev(xh_, z_, core_, xl_, y_):
        return {"dp": (xh_ * NZ + z_) * 2 + core_, "tensor": xl_ * NY + y_}

    def zat(r):
        return lax.rem(z + sgn * r + 2 * NZ, NZ)

    def yat(r):
        return lax.rem(y + sgn * r + 2 * NY, NY)

    sibling = dev(xh, z, 1 - core, xl, y)
    partner = dev(xh, z, core, 1 - xl, y)
    across = dev(1 - xh, z, core, 1 - xl, y)

    loads = []
    for k in range(KC):
        cols = pl.ds(k * KW, KW)
        loads.append((
            pltpu.make_async_copy(x_hbm.at[:, cols], x_v.at[:, cols], lsem.at[k]),
            pltpu.make_async_copy(w_hbm.at[:, cols], w_v.at[:, cols], lsem.at[KC + k]),
        ))
    for a, b in loads:
        a.start()
        b.start()
    qg_load = pltpu.make_async_copy(qg_hbm, qg_v, lsem.at[L_QG])
    qg_load.start()
    gain_load = pltpu.make_async_copy(gain_hbm, gain_v, lsem.at[L_GAIN])
    gain_load.start()
    myhalf = pl.ds(pl.multiple_of(xl * HALF, 128), HALF)
    wh_load = pltpu.make_async_copy(w_hbm.at[:, myhalf], wst_v.at[:F], lsem.at[L_WH])
    wh_load.start()

    barrier = pltpu.get_barrier_semaphore()
    peers = [{"dp": d, "tensor": lax.rem(t + o, NT)} for o in range(1, NT)]
    peers += [across, sibling]
    peers += [dev(xh, zat(r), core, xl, y) for r in (1, -1, 2, -2, 5, -5)]
    peers += [dev(1 - xh, zat(r), core, xl, y) for r in (0, 1, -1, 2, -2)]
    for p in peers:
        pl.semaphore_signal(barrier, inc=1, device_id=p, device_id_type=MESH)

    pt = None
    for k, (a, b) in enumerate(loads):
        a.wait()
        b.wait()
        cols = slice(k * KW, (k + 1) * KW)
        term = dot(w_v[:, cols], x_v[:, cols], ((1,), (1,)))
        pt = term if pt is None else pt + term
    qg_load.wait()
    gain_load.wait()
    rows = lax.broadcasted_iota(jnp.int32, (F, F), 0)
    lanes = lax.broadcasted_iota(jnp.int32, (F, F), 1)
    gain = jnp.sum(jnp.where(rows == lanes, gain_v[...], 0.0), axis=1, keepdims=True)
    sg = qg_v[...].astype(F32) * gain
    sq = jnp.sum(pt * pt, axis=0, keepdims=True)
    cr = jnp.sum(sg * pt, axis=0, keepdims=True)
    sums_v[t, 0:1, :] = sq[:, :128]
    sums_v[t, 1:2, :] = sq[:, 128:]
    sums_v[t, 2:3, :] = cr[:, :128]
    sums_v[t, 3:4, :] = cr[:, 128:]

    pl.semaphore_wait(barrier, len(peers))

    def send(src, dst, ssem_at, rsem_at, device):
        pltpu.make_async_remote_copy(
            src_ref=src, dst_ref=dst, send_sem=ssem.at[ssem_at], recv_sem=rsem.at[rsem_at],
            device_id=device, device_id_type=MESH,
        ).start()

    def handle(ref, ssem_at, rsem_at):
        return pltpu.make_async_remote_copy(
            src_ref=ref, dst_ref=ref, send_sem=ssem.at[ssem_at], recv_sem=rsem.at[rsem_at],
            device_id=sibling, device_id_type=MESH,
        )

    def arrived(ref, rsem_at):
        handle(ref, 0, rsem_at).wait_recv()

    def left(ref, ssem_at):
        handle(ref, ssem_at, 0).wait_send()

    for p in peers[: NT - 1]:
        send(sums_v.at[t], sums_v.at[t], S_SUMS, SUMS, p)

    wpart = wst_v.at[F:]
    for n, who in enumerate((partner, across)):
        src = pl.ds(pl.multiple_of((1 - xl) * HALF + (2 * n + core) * CS, 128), CS)
        dst = pl.ds(pl.multiple_of((2 * n + core) * CS, 128), CS)
        send(w_v.at[:, src], wpart.at[:, dst], S_WX, WX + n, who)

    for k in range(D // 256):
        turned = x_v[:, k * 256 : (k + 1) * 256].T
        at, end = k * 256, (k + 1) * 256
        while at < end:
            h, zz, o = at // HALF, at % HALF // 160, at % 160
            n = min(160 - o, end - at)
            xt_v[zz, h * 160 + o : h * 160 + o + n, :] = turned[at - k * 256 : at - k * 256 + n]
            at += n
    pga_v[F:, :] = jnp.zeros((256 - F, T), BF16)
    sgt_v[...] = sg.T
    ptt_v[...] = pt.T

    arrived(sums_v.at[: NT - 1], SUMS)
    total = sums_v[0]
    for s in range(1, NT):
        total = total + sums_v[s]
    sq = jnp.concatenate([total[0:1], total[1:2]], axis=1)
    cr = jnp.concatenate([total[2:3], total[3:4]], axis=1)
    inv = 1.0 / jnp.sqrt(sq / HQ + epsilon)
    coef = inv * inv * inv * (cr / HQ)
    pg = (inv * sg - coef * pt).astype(BF16)
    pga_v[:F, :] = pg
    send(pga_v.at[:F], pgp_v, S_PG, PG, partner)

    def blocks(g):
        for r in GROUPS[g]:
            v = dot(xt_v[zat(r)], pga_v[...], ((1,), (1,)))
            mirror = r if r in (0, 8) else -r
            for h in (0, 1):
                a, b = v[h * 160 : h * 160 + 80], v[h * 160 + 80 : h * 160 + 160]
                mine = packed(jnp.where(core == 0, a, b))
                other = packed(jnp.where(core == 0, b, a))
                for ref, i, parts in ((own_v, AT[r], mine), (dsend, AT[mirror], other)):
                    ref[i, h, :80, :] = parts[0].astype(ref.dtype)
                    ref[i, h, 80:96, :] = parts[1].astype(ref.dtype)
                    ref[i, h, 96:, :] = parts[2].astype(ref.dtype)
        at = pl.ds(AT[GROUPS[g][0]], len(GROUPS[g]))
        send(dsend.at[at], drecv.at[at], S_DD, DD + g, sibling)

    def local(r, h):
        return own_v[AT[r], h] + drecv[AT[r], h].astype(F32)

    def zcross(r, v):
        zs_v[AT[r], 1 - xh] = v.astype(BF16)
        send(
            zs_v.at[AT[r], 1 - xh], zrecv.at[SLOT["cross", r]], S_Z, ZC + JOINS.index(CROSS[r]),
            dev(1 - xh, zat(r - CROSS[r]), core, xl, y),
        )

    def zown(r, v):
        zs_v[AT[r], xh] = v.astype(BF16)
        send(
            zs_v.at[AT[r], xh], zrecv.at[SLOT["own", r]], S_Z, ZC + JOINS.index(PARENT[r]),
            dev(xh, zat(r - PARENT[r]), core, xl, y),
        )

    def zboth(r, pair):
        for h, v in enumerate(pair):
            zs_v[AT[r], h] = v.astype(BF16)
        send(
            zs_v.at[AT[r]], zrecv.at[pl.ds(SLOT["own", r], 2)], S_Z, ZC + JOINS.index(PARENT[r]),
            dev(xh, zat(r - PARENT[r]), core, xl, y),
        )

    def zleaf(g):
        at = pl.ds(AT[GROUPS[g][0]], len(GROUPS[g]))
        arrived(drecv.at[at], DD + g)
        for r in GROUPS[g]:
            if abs(r) >= 5 or r == 0:
                zcross(r, local(r, 1 - xh))
            if r not in JOINS:
                if abs(r) >= 5:
                    zown(r, local(r, xh))
                else:
                    zboth(r, [local(r, h) for h in (0, 1)])

    def joined(r):
        first, n = JOIN_SLOTS[r]
        arrived(zrecv.at[pl.ds(first, n)], ZC + JOINS.index(r))
        slots = range(first, first + n)
        if abs(r) >= 5 or r == 0:
            v = local(r, xh)
            for k in slots:
                v = v + zrecv[k].astype(F32)
            return v
        pair = []
        for h in ((0, 1) if abs(r) == 3 else (xh, 1 - xh)):
            v = local(r, h)
            for k in range(first, first + n, 2):
                v = v + zrecv[k + h].astype(F32)
            pair.append(v)
        return pair

    def zjoin(r):
        v = joined(r)
        if abs(r) == 5 or r == 7:
            zown(r, v)
        elif abs(r) == 3:
            zboth(r, v)
        else:
            zcross(r, v[1])
            zown(r, v[0])

    def yrows(r):
        return pl.multiple_of(yat(r) * 16, 16)

    def mine(r, s, h):
        return part_v[s, pl.ds(yrows(r) + h * 128, 16), :]

    def ylast_send(slot, s, rows, dest):
        for i, who in enumerate((xl, 1 - xl)):
            if dest is None and i == 0:
                continue
            src = rows.at[pl.ds(pl.multiple_of(who * 16, 16), 16)]
            send(src, yfin.at[s, slot + i], S_YF, YF + s, dev(xh, z, core, who, y if dest is None else dest))

    def ystep(k, s):
        for r in YSTEPS[k]:
            new = [mine(r, s, h) for h in (0, 1)]
            if r not in YHEADS:
                slot = YSLOT[r]
                arrived(yrecv.at[slot, s], YC + slot * S + s)
                new = [v + yrecv[slot, s, h * 16 : h * 16 + 16, :].astype(F32) for h, v in enumerate(new)]
            to = yat(1 if r > 0 else -1)
            if abs(r) == 1:
                rows = ylast.at[0 if r > 0 else 1, s]
            else:
                slot = YSLOT[r - 1 if r > 0 else r + 1]
                rows = ysend.at[slot, s]
            for h, v in enumerate(new):
                rows[h * 16 : h * 16 + 16, :] = v.astype(BF16)
            if abs(r) == 1:
                ylast_send(0 if r > 0 else 2, s, rows, to)
            else:
                send(rows, yrecv.at[slot, s], S_Y, YC + slot * S + s, dev(xh, z, core, xl, to))

    def yown_cross(s):
        for h in (0, 1):
            ylast[2, s, h * 16 : h * 16 + 16, :] = mine(0, s, h).astype(BF16)
        ylast_send(3, s, ylast.at[2, s], None)

    blocks(0)
    blocks(1)
    for n in (0, 1):
        cols = pl.ds(pl.multiple_of((2 * n + core) * CS, 128), CS)
        arrived(wpart.at[:, cols], WX + n)
        send(wpart.at[:, cols], wpart.at[:, cols], S_WD, WD + n, sibling)
    wh_load.wait()
    both = jnp.concatenate([inv, coef], axis=0)
    both = jnp.concatenate([both, jnp.zeros((6, T), F32)], axis=0).T
    own = (both[:, 0:1] * sgt_v[...] - both[:, 1:2] * ptt_v[...]).astype(BF16)
    for s in range(S):
        part_v[s] = dot(own, wst_v[:F, s * CS : (s + 1) * CS], ((1,), (0,)))
    zleaf(0)
    zleaf(1)
    blocks(2)
    arrived(pgp_v, PG)
    theirs = pgp_v[...].T
    for n in (0, 1):
        cols = pl.ds(pl.multiple_of((2 * n + 1 - core) * CS, 128), CS)
        arrived(wpart.at[:, cols], WD + n)
    for s in range(S):
        part_v[s] += dot(theirs, wst_v[F:, s * CS : (s + 1) * CS], ((1,), (0,)))
        ystep(0, s)
    for s in range(S):
        yown_cross(s)
    zleaf(2)
    blocks(3)
    zleaf(3)
    zjoin(7)
    for s in range(S):
        ystep(1, s)
    zjoin(3)
    zjoin(-3)
    zjoin(-5)
    zjoin(5)
    for s in range(S):
        ystep(2, s)
    for s in range(S):
        ystep(3, s)
    zjoin(1)
    zjoin(-1)
    outs = []
    for s in range(S):
        arrived(yfin.at[s], YF + s)
        own = part_v[s, pl.ds(yrows(0) + xl * 128, 16), :]
        for who, v, slots in ((xl, own, (0, 2)), (1 - xl, 0.0, (1, 3, 4))):
            for slot in slots:
                v = v + yfin[s, slot].astype(F32)
            cols = pl.ds(pl.multiple_of(who * HALF + s * CS, 128), CS)
            out_v[:, cols] = v.astype(BF16)
            pltpu.make_async_copy(out_v.at[:, cols], ig_hbm.at[:, cols], lsem.at[L_OUT]).start()

    v = joined(0)
    wg_v[:, :128] = v[:80]
    wg_v[:16, 128:] = v[80:96, :32]
    for j in (1, 2, 3):
        wg_v[16 * j : 16 * j + 16, 128:] = pltpu.roll(v[80:96], 128 - 32 * j, 1)[:, :32]
    wg_v[64:, 128:] = v[96:, :32]
    outs.append(pltpu.make_async_copy(wg_v, wg_hbm, lsem.at[L_OUT + 1]))
    outs[0].start()

    left(sums_v.at[: NT - 1], S_SUMS)
    left(wpart.at[:, : 2 * CS], S_WX)
    left(wpart.at[:, : 2 * CS], S_WD)
    left(pgp_v, S_PG)
    left(dsend, S_DD)
    left(zrecv, S_Z)
    left(yrecv, S_Y)
    left(yfin, S_YF)
    outs.append(pltpu.make_async_copy(out_v, ig_hbm, lsem.at[L_OUT]))
    for copy in outs:
        copy.wait()


def per_device(block_input, query_weight, query_gain, query_grad):
    hbm = pl.BlockSpec(memory_space=pltpu.HBM)
    anywhere = pl.BlockSpec(memory_space=pl.ANY)
    return pl.pallas_call(
        kernel,
        out_shape=(
            jax.ShapeDtypeStruct((T // NT, D), BF16),
            jax.ShapeDtypeStruct((80, F), F32),
        ),
        in_specs=[hbm, hbm, hbm, hbm],
        out_specs=(anywhere, anywhere),
        scratch_shapes=[
            pltpu.VMEM((T, D), BF16),
            pltpu.VMEM((NZ, 320, T), BF16),
            pltpu.VMEM((F, D), BF16),
            pltpu.VMEM((2 * F, HALF), BF16),
            pltpu.VMEM((1, F), F32),
            pltpu.VMEM((F, T), BF16),
            pltpu.VMEM((NT, 4, 128), F32),
            pltpu.VMEM((256, T), BF16),
            pltpu.VMEM((F, T), BF16),
            pltpu.VMEM((T, F), F32),
            pltpu.VMEM((T, F), F32),
            pltpu.VMEM((16, 2, PACK, 128), BF16),
            pltpu.VMEM((16, 2, PACK, 128), BF16),
            pltpu.VMEM((16, 2, PACK, 128), F32),
            pltpu.VMEM((16, 2, PACK, 128), BF16),
            pltpu.VMEM((NSLOT, PACK, 128), BF16),
            pltpu.VMEM((80, F), F32),
            pltpu.VMEM((S, T, CS), F32),
            pltpu.VMEM((5, S, 32, CS), BF16),
            pltpu.VMEM((5, S, 32, CS), BF16),
            pltpu.VMEM((3, S, 32, CS), BF16),
            pltpu.VMEM((S, 5, 16, CS), BF16),
            pltpu.VMEM((T // NT, D), BF16),
            pltpu.SemaphoreType.DMA((L_OUT + 3,)),
            pltpu.SemaphoreType.DMA((8,)),
            pltpu.SemaphoreType.DMA((NRECV,)),
        ],
        compiler_params=pltpu.CompilerParams(
            collective_id=0, has_side_effects=True, vmem_limit_bytes=40 * 1024 * 1024
        ),
    )(*(pltpu.with_memory_space_constraint(a, pltpu.HBM) for a in (block_input, query_weight, query_gain.reshape(1, F), query_grad)))


def solution(mesh):
    return jax.shard_map(
        per_device,
        mesh=mesh,
        in_specs=(P("dp", None), P("tensor", None), P("tensor"), P("tensor", "dp")),
        out_specs=(P(("dp", "tensor"), None), P("dp", "tensor")),
        check_vma=False,
    )
```

```python
import jax
import jax.numpy as jnp
from jax import lax
from jax.experimental import pallas as pl
from jax.experimental.pallas import tpu as pltpu
from jax.sharding import PartitionSpec as P

MESH = pl.DeviceIdType.MESH
F32, BF16 = jnp.float32, jnp.bfloat16

NT, NY, NZ = 16, 8, 16
T, F, D = 256, 160, 5120
HALF = D // 2
S = 4
CS = HALF // S
KC = 8
KW = D // KC
HQ = F * NT
epsilon = 1e-6

PARENT = {8: 6, 7: 6, 6: 4, 5: 4, 4: 0, 3: 1, 2: 1, 1: 0, -7: -6, -6: -4, -5: -4, -4: 0, -3: -1, -2: -1, -1: 0}
CROSS = {8: 6, 7: 6, 6: 6, 5: 4, 4: 4, -7: -6, -6: -6, -5: -4, -4: -4, 1: 0, -1: 0, 0: 0}
GROUPS = ((8, 7, -7), (6, -6, 5, -5), (4, -4, 3, -3), (2, -2, 1, -1, 0))
ORDER = sum(GROUPS, ())
AT = {r: i for i, r in enumerate(ORDER)}
JOINS = (6, -6, 4, -4, 1, -1, 0)
FAR = 4
SLOT, JOIN_SLOTS = {}, {}
count = 0
for j in JOINS:
    first = count
    for r in ORDER:
        if PARENT.get(r) == j:
            SLOT["own", r] = count
            count += 2 if abs(r) < FAR and j else 1
        if CROSS.get(r) == j:
            SLOT["cross", r] = count
            count += 1
    JOIN_SLOTS[j] = (first, count - first)
NSLOT = count
PACK = 112

YSTEPS = ((4, -3), (3, -2), (2, -1), (1,))
YHEADS = (4, -3)
YSLOT = {3: 0, 2: 1, 1: 2, -2: 3, -1: 4}

SUMS, WX, WD, PG = 0, 1, 3, 5
DD = 6
ZC = DD + len(GROUPS)
YC = ZC + len(JOINS)
YF = YC + 5 * S
NRECV = YF + S
S_SUMS, S_WX, S_WD, S_PG, S_DD, S_Z, S_Y, S_YF = range(8)
L_QG, L_GAIN, L_WH, L_OUT = 2 * KC, 2 * KC + 1, 2 * KC + 2, 2 * KC + 3


def dot(a, b, dims):
    return lax.dot_general(a, b, (dims, ((), ())), preferred_element_type=F32)


def packed(v):
    rest = v[:, 128:]
    tile = rest[:16]
    for j in (1, 2, 3):
        tile = tile + pltpu.roll(rest[16 * j : 16 * j + 16], 32 * j, 1)
    return v[:, :128], tile, rest[64:]


def kernel(
    x_hbm, w_hbm, gain_hbm, qg_hbm, ig_hbm, wg_hbm,
    x_v, xt_v, w_v, wst_v, gain_v, qg_v, sums_v, pga_v, pgp_v, sgt_v, ptt_v,
    dsend, drecv, own_v, zs_v, zrecv, wg_v,
    part_v, ysend, yrecv, ylast, yfin, out_v,
    lsem, ssem, rsem,
):
    d = lax.axis_index("dp")
    t = lax.axis_index("tensor")
    core = lax.rem(d, 2)
    z = lax.rem(lax.div(d, 2), NZ)
    xh = lax.div(d, 2 * NZ)
    y = lax.rem(t, NY)
    xl = lax.div(t, NY)
    sgn = 1 - 2 * core

    def dev(xh_, z_, core_, xl_, y_):
        return {"dp": (xh_ * NZ + z_) * 2 + core_, "tensor": xl_ * NY + y_}

    def zat(r):
        return lax.rem(z + sgn * r + 2 * NZ, NZ)

    def yat(r):
        return lax.rem(y + sgn * r + 2 * NY, NY)

    sibling = dev(xh, z, 1 - core, xl, y)
    partner = dev(xh, z, core, 1 - xl, y)
    across = dev(1 - xh, z, core, 1 - xl, y)

    loads = []
    for k in range(KC):
        cols = pl.ds(k * KW, KW)
        loads.append((
            pltpu.make_async_copy(x_hbm.at[:, cols], x_v.at[:, cols], lsem.at[k]),
            pltpu.make_async_copy(w_hbm.at[:, cols], w_v.at[:, cols], lsem.at[KC + k]),
        ))
    for a, b in loads:
        a.start()
        b.start()
    qg_load = pltpu.make_async_copy(qg_hbm, qg_v, lsem.at[L_QG])
    qg_load.start()
    gain_load = pltpu.make_async_copy(gain_hbm, gain_v, lsem.at[L_GAIN])
    gain_load.start()
    myhalf = pl.ds(pl.multiple_of(xl * HALF, 128), HALF)
    wh_load = pltpu.make_async_copy(w_hbm.at[:, myhalf], wst_v.at[:F], lsem.at[L_WH])
    wh_load.start()

    barrier = pltpu.get_barrier_semaphore()
    peers = [{"dp": d, "tensor": lax.rem(t + o, NT)} for o in range(1, NT)]
    peers += [across, sibling]
    peers += [dev(xh, zat(r), core, xl, y) for r in (1, -1, 2, -2, 4, -4)]
    peers += [dev(1 - xh, zat(r), core, xl, y) for r in (0, 1, -1, 2, -2)]
    for p in peers:
        pl.semaphore_signal(barrier, inc=1, device_id=p, device_id_type=MESH)

    pt = None
    for k, (a, b) in enumerate(loads):
        a.wait()
        b.wait()
        cols = slice(k * KW, (k + 1) * KW)
        term = dot(w_v[:, cols], x_v[:, cols], ((1,), (1,)))
        pt = term if pt is None else pt + term
    qg_load.wait()
    gain_load.wait()
    rows = lax.broadcasted_iota(jnp.int32, (F, F), 0)
    lanes = lax.broadcasted_iota(jnp.int32, (F, F), 1)
    gain = jnp.sum(jnp.where(rows == lanes, gain_v[...], 0.0), axis=1, keepdims=True)
    sg = qg_v[...].astype(F32) * gain
    sq = jnp.sum(pt * pt, axis=0, keepdims=True)
    cr = jnp.sum(sg * pt, axis=0, keepdims=True)
    sums_v[t, 0:1, :] = sq[:, :128]
    sums_v[t, 1:2, :] = sq[:, 128:]
    sums_v[t, 2:3, :] = cr[:, :128]
    sums_v[t, 3:4, :] = cr[:, 128:]

    pl.semaphore_wait(barrier, len(peers))

    def send(src, dst, ssem_at, rsem_at, device):
        pltpu.make_async_remote_copy(
            src_ref=src, dst_ref=dst, send_sem=ssem.at[ssem_at], recv_sem=rsem.at[rsem_at],
            device_id=device, device_id_type=MESH,
        ).start()

    def handle(ref, ssem_at, rsem_at):
        return pltpu.make_async_remote_copy(
            src_ref=ref, dst_ref=ref, send_sem=ssem.at[ssem_at], recv_sem=rsem.at[rsem_at],
            device_id=sibling, device_id_type=MESH,
        )

    def arrived(ref, rsem_at):
        handle(ref, 0, rsem_at).wait_recv()

    def left(ref, ssem_at):
        handle(ref, ssem_at, 0).wait_send()

    for p in peers[: NT - 1]:
        send(sums_v.at[t], sums_v.at[t], S_SUMS, SUMS, p)

    wpart = wst_v.at[F:]
    for n, who in enumerate((partner, across)):
        src = pl.ds(pl.multiple_of((1 - xl) * HALF + (2 * n + core) * CS, 128), CS)
        dst = pl.ds(pl.multiple_of((2 * n + core) * CS, 128), CS)
        send(w_v.at[:, src], wpart.at[:, dst], S_WX, WX + n, who)

    for k in range(D // 256):
        turned = x_v[:, k * 256 : (k + 1) * 256].T
        at, end = k * 256, (k + 1) * 256
        while at < end:
            h, zz, o = at // HALF, at % HALF // 160, at % 160
            n = min(160 - o, end - at)
            xt_v[zz, h * 160 + o : h * 160 + o + n, :] = turned[at - k * 256 : at - k * 256 + n]
            at += n
    pga_v[F:, :] = jnp.zeros((256 - F, T), BF16)
    sgt_v[...] = sg.T
    ptt_v[...] = pt.T

    arrived(sums_v.at[: NT - 1], SUMS)
    total = sums_v[0]
    for s in range(1, NT):
        total = total + sums_v[s]
    sq = jnp.concatenate([total[0:1], total[1:2]], axis=1)
    cr = jnp.concatenate([total[2:3], total[3:4]], axis=1)
    inv = 1.0 / jnp.sqrt(sq / HQ + epsilon)
    coef = inv * inv * inv * (cr / HQ)
    pg = (inv * sg - coef * pt).astype(BF16)
    pga_v[:F, :] = pg
    send(pga_v.at[:F], pgp_v, S_PG, PG, partner)

    def blocks(g):
        for r in GROUPS[g]:
            v = dot(xt_v[zat(r)], pga_v[...], ((1,), (1,)))
            mirror = r if r in (0, 8) else -r
            for h in (0, 1):
                a, b = v[h * 160 : h * 160 + 80], v[h * 160 + 80 : h * 160 + 160]
                mine = packed(jnp.where(core == 0, a, b))
                other = packed(jnp.where(core == 0, b, a))
                for ref, i, parts in ((own_v, AT[r], mine), (dsend, AT[mirror], other)):
                    ref[i, h, :80, :] = parts[0].astype(ref.dtype)
                    ref[i, h, 80:96, :] = parts[1].astype(ref.dtype)
                    ref[i, h, 96:, :] = parts[2].astype(ref.dtype)
        at = pl.ds(AT[GROUPS[g][0]], len(GROUPS[g]))
        send(dsend.at[at], drecv.at[at], S_DD, DD + g, sibling)

    def local(r, h):
        return own_v[AT[r], h] + drecv[AT[r], h].astype(F32)

    def zcross(r, v):
        zs_v[AT[r], 1 - xh] = v.astype(BF16)
        send(
            zs_v.at[AT[r], 1 - xh], zrecv.at[SLOT["cross", r]], S_Z, ZC + JOINS.index(CROSS[r]),
            dev(1 - xh, zat(r - CROSS[r]), core, xl, y),
        )

    def zown(r, v):
        zs_v[AT[r], xh] = v.astype(BF16)
        send(
            zs_v.at[AT[r], xh], zrecv.at[SLOT["own", r]], S_Z, ZC + JOINS.index(PARENT[r]),
            dev(xh, zat(r - PARENT[r]), core, xl, y),
        )

    def zboth(r, pair):
        for h, v in enumerate(pair):
            zs_v[AT[r], h] = v.astype(BF16)
        send(
            zs_v.at[AT[r]], zrecv.at[pl.ds(SLOT["own", r], 2)], S_Z, ZC + JOINS.index(PARENT[r]),
            dev(xh, zat(r - PARENT[r]), core, xl, y),
        )

    def zleaf(g):
        at = pl.ds(AT[GROUPS[g][0]], len(GROUPS[g]))
        arrived(drecv.at[at], DD + g)
        for r in GROUPS[g]:
            if abs(r) >= FAR or r == 0:
                zcross(r, local(r, 1 - xh))
            if r not in JOINS:
                if abs(r) >= FAR:
                    zown(r, local(r, xh))
                else:
                    zboth(r, [local(r, h) for h in (0, 1)])

    def joined(r):
        first, n = JOIN_SLOTS[r]
        arrived(zrecv.at[pl.ds(first, n)], ZC + JOINS.index(r))
        slots = range(first, first + n)
        if abs(r) >= FAR or r == 0:
            v = local(r, xh)
            for k in slots:
                v = v + zrecv[k].astype(F32)
            return v
        pair = []
        for h in (xh, 1 - xh):
            v = local(r, h)
            for k in range(first, first + n, 2):
                v = v + zrecv[k + h].astype(F32)
            pair.append(v)
        return pair

    def zjoin(r):
        v = joined(r)
        if abs(r) >= FAR:
            zown(r, v)
        else:
            zcross(r, v[1])
            zown(r, v[0])

    def yrows(r):
        return pl.multiple_of(yat(r) * 16, 16)

    def mine(r, s, h):
        return part_v[s, pl.ds(yrows(r) + h * 128, 16), :]

    def ylast_send(slot, s, rows, dest):
        for i, who in enumerate((xl, 1 - xl)):
            if dest is None and i == 0:
                continue
            src = rows.at[pl.ds(pl.multiple_of(who * 16, 16), 16)]
            send(src, yfin.at[s, slot + i], S_YF, YF + s, dev(xh, z, core, who, y if dest is None else dest))

    def ystep(k, s):
        for r in YSTEPS[k]:
            new = [mine(r, s, h) for h in (0, 1)]
            if r not in YHEADS:
                slot = YSLOT[r]
                arrived(yrecv.at[slot, s], YC + slot * S + s)
                new = [v + yrecv[slot, s, h * 16 : h * 16 + 16, :].astype(F32) for h, v in enumerate(new)]
            to = yat(1 if r > 0 else -1)
            if abs(r) == 1:
                rows = ylast.at[0 if r > 0 else 1, s]
            else:
                slot = YSLOT[r - 1 if r > 0 else r + 1]
                rows = ysend.at[slot, s]
            for h, v in enumerate(new):
                rows[h * 16 : h * 16 + 16, :] = v.astype(BF16)
            if abs(r) == 1:
                ylast_send(0 if r > 0 else 2, s, rows, to)
            else:
                send(rows, yrecv.at[slot, s], S_Y, YC + slot * S + s, dev(xh, z, core, xl, to))

    def yown_cross(s):
        for h in (0, 1):
            ylast[2, s, h * 16 : h * 16 + 16, :] = mine(0, s, h).astype(BF16)
        ylast_send(3, s, ylast.at[2, s], None)

    blocks(0)
    blocks(1)
    for n in (0, 1):
        cols = pl.ds(pl.multiple_of((2 * n + core) * CS, 128), CS)
        arrived(wpart.at[:, cols], WX + n)
        send(wpart.at[:, cols], wpart.at[:, cols], S_WD, WD + n, sibling)
    wh_load.wait()
    both = jnp.concatenate([inv, coef], axis=0)
    both = jnp.concatenate([both, jnp.zeros((6, T), F32)], axis=0).T
    own = (both[:, 0:1] * sgt_v[...] - both[:, 1:2] * ptt_v[...]).astype(BF16)
    for s in range(S):
        part_v[s] = dot(own, wst_v[:F, s * CS : (s + 1) * CS], ((1,), (0,)))
    zleaf(0)
    zleaf(1)
    arrived(pgp_v, PG)
    theirs = pgp_v[...].T
    for n in (0, 1):
        cols = pl.ds(pl.multiple_of((2 * n + 1 - core) * CS, 128), CS)
        arrived(wpart.at[:, cols], WD + n)
    for s in range(S):
        part_v[s] += dot(theirs, wst_v[F:, s * CS : (s + 1) * CS], ((1,), (0,)))
        ystep(0, s)
    for s in range(S):
        yown_cross(s)
    blocks(2)
    blocks(3)
    zleaf(2)
    zleaf(3)
    for s in (0, 1):
        ystep(1, s)
    zjoin(6)
    zjoin(-6)
    for s in (2, 3):
        ystep(1, s)
    for s in (0, 1):
        ystep(2, s)
    for s in (2, 3):
        ystep(2, s)
    zjoin(1)
    zjoin(-1)
    zjoin(4)
    zjoin(-4)
    for s in (0, 1):
        ystep(3, s)
    for s in (2, 3):
        ystep(3, s)
    outs = []
    for s in range(S):
        arrived(yfin.at[s], YF + s)
        own = part_v[s, pl.ds(yrows(0) + xl * 128, 16), :]
        for who, v, slots in ((xl, own, (0, 2)), (1 - xl, 0.0, (1, 3, 4))):
            for slot in slots:
                v = v + yfin[s, slot].astype(F32)
            cols = pl.ds(pl.multiple_of(who * HALF + s * CS, 128), CS)
            out_v[:, cols] = v.astype(BF16)
            pltpu.make_async_copy(out_v.at[:, cols], ig_hbm.at[:, cols], lsem.at[L_OUT]).start()

    v = joined(0)
    wg_v[:, :128] = v[:80]
    wg_v[:16, 128:] = v[80:96, :32]
    for j in (1, 2, 3):
        wg_v[16 * j : 16 * j + 16, 128:] = pltpu.roll(v[80:96], 128 - 32 * j, 1)[:, :32]
    wg_v[64:, 128:] = v[96:, :32]
    outs.append(pltpu.make_async_copy(wg_v, wg_hbm, lsem.at[L_OUT + 1]))
    outs[0].start()

    left(sums_v.at[: NT - 1], S_SUMS)
    left(wpart.at[:, : 2 * CS], S_WX)
    left(wpart.at[:, : 2 * CS], S_WD)
    left(pgp_v, S_PG)
    left(dsend, S_DD)
    left(zrecv, S_Z)
    left(yrecv, S_Y)
    left(yfin, S_YF)
    outs.append(pltpu.make_async_copy(out_v, ig_hbm, lsem.at[L_OUT]))
    for copy in outs:
        copy.wait()


def per_device(block_input, query_weight, query_gain, query_grad):
    hbm = pl.BlockSpec(memory_space=pltpu.HBM)
    anywhere = pl.BlockSpec(memory_space=pl.ANY)
    return pl.pallas_call(
        kernel,
        out_shape=(
            jax.ShapeDtypeStruct((T // NT, D), BF16),
            jax.ShapeDtypeStruct((80, F), F32),
        ),
        in_specs=[hbm, hbm, hbm, hbm],
        out_specs=(anywhere, anywhere),
        scratch_shapes=[
            pltpu.VMEM((T, D), BF16),
            pltpu.VMEM((NZ, 320, T), BF16),
            pltpu.VMEM((F, D), BF16),
            pltpu.VMEM((2 * F, HALF), BF16),
            pltpu.VMEM((1, F), F32),
            pltpu.VMEM((F, T), BF16),
            pltpu.VMEM((NT, 4, 128), F32),
            pltpu.VMEM((256, T), BF16),
            pltpu.VMEM((F, T), BF16),
            pltpu.VMEM((T, F), F32),
            pltpu.VMEM((T, F), F32),
            pltpu.VMEM((16, 2, PACK, 128), BF16),
            pltpu.VMEM((16, 2, PACK, 128), BF16),
            pltpu.VMEM((16, 2, PACK, 128), F32),
            pltpu.VMEM((16, 2, PACK, 128), BF16),
            pltpu.VMEM((NSLOT, PACK, 128), BF16),
            pltpu.VMEM((80, F), F32),
            pltpu.VMEM((S, T, CS), F32),
            pltpu.VMEM((5, S, 32, CS), BF16),
            pltpu.VMEM((5, S, 32, CS), BF16),
            pltpu.VMEM((3, S, 32, CS), BF16),
            pltpu.VMEM((S, 5, 16, CS), BF16),
            pltpu.VMEM((T // NT, D), BF16),
            pltpu.SemaphoreType.DMA((L_OUT + 3,)),
            pltpu.SemaphoreType.DMA((8,)),
            pltpu.SemaphoreType.DMA((NRECV,)),
        ],
        compiler_params=pltpu.CompilerParams(
            collective_id=0, has_side_effects=True, vmem_limit_bytes=40 * 1024 * 1024
        ),
    )(*(pltpu.with_memory_space_constraint(a, pltpu.HBM) for a in (block_input, query_weight, query_gain.reshape(1, F), query_grad)))


def solution(mesh):
    return jax.shard_map(
        per_device,
        mesh=mesh,
        in_specs=(P("dp", None), P("tensor", None), P("tensor"), P("tensor", "dp")),
        out_specs=(P(("dp", "tensor"), None), P("dp", "tensor")),
        check_vma=False,
    )
```

```python
import jax
import jax.numpy as jnp
from jax import lax
from jax.experimental import pallas as pl
from jax.experimental.pallas import tpu as pltpu
from jax.sharding import PartitionSpec as P

MESH = pl.DeviceIdType.MESH
F32, BF16 = jnp.float32, jnp.bfloat16

NT, NY, NZ = 16, 8, 16
T, F, D = 256, 160, 5120
HALF = D // 2
S = 4
CS = HALF // S
KC = 8
KW = D // KC
HQ = F * NT
epsilon = 1e-6

PARENT = {8: 6, 7: 6, 6: 4, 5: 4, 4: 0, 3: 1, 2: 1, 1: 0, -7: -6, -6: -4, -5: -4, -4: 0, -3: -1, -2: -1, -1: 0}
CROSS = {8: 6, 7: 6, 6: 6, 5: 4, 4: 4, -7: -6, -6: -6, -5: -4, -4: -4, 1: 0, -1: 0, 0: 0}
GROUPS = ((8, 7, -7), (6, -6, 5, -5), (4, -4, 3, -3), (2, -2, 1, -1, 0))
ORDER = sum(GROUPS, ())
AT = {r: i for i, r in enumerate(ORDER)}
JOINS = (6, -6, 4, -4, 1, -1, 0)
FAR = 4
SLOT, JOIN_SLOTS = {}, {}
count = 0
for j in JOINS:
    first = count
    for r in ORDER:
        if PARENT.get(r) == j:
            SLOT["own", r] = count
            count += 2 if abs(r) < FAR and j else 1
        if CROSS.get(r) == j:
            SLOT["cross", r] = count
            count += 1
    JOIN_SLOTS[j] = (first, count - first)
NSLOT = count
PACK = 112

YSTEPS = ((4, -3), (3, -2), (2, -1), (1,))
YHEADS = (4, -3)
YSLOT = {3: 0, 2: 1, 1: 2, -2: 3, -1: 4}

SUMS, WX, WD, PG = 0, 1, 3, 5
DD = 6
ZC = DD + len(GROUPS)
YC = ZC + len(JOINS)
YF = YC + 5 * S
NRECV = YF + S
S_SUMS, S_WX, S_WD, S_PG, S_DD, S_Z, S_Y, S_YF = range(8)
L_QG, L_GAIN, L_WH = KC, KC + 1, KC + 2


def dot(a, b, dims):
    return lax.dot_general(a, b, (dims, ((), ())), preferred_element_type=F32)


def packed(v):
    rest = v[:, 128:]
    tile = rest[:16]
    for j in (1, 2, 3):
        tile = tile + pltpu.roll(rest[16 * j : 16 * j + 16], 32 * j, 1)
    return v[:, :128], tile, rest[64:]


def kernel(
    x_hbm, w_hbm, gain_hbm, qg_hbm, out_v, wg_v,
    xw_v, xt_v, wst_v, gain_v, qg_v, sums_v, pga_v, pgp_v, sgt_v, ptt_v,
    dsend, drecv, own_v, zs_v, zrecv,
    part_v, ysend, yrecv, ylast, yfin,
    lsem, ssem, rsem,
):
    d = lax.axis_index("dp")
    t = lax.axis_index("tensor")
    core = lax.rem(d, 2)
    z = lax.rem(lax.div(d, 2), NZ)
    xh = lax.div(d, 2 * NZ)
    y = lax.rem(t, NY)
    xl = lax.div(t, NY)
    sgn = 1 - 2 * core

    def dev(xh_, z_, core_, xl_, y_):
        return {"dp": (xh_ * NZ + z_) * 2 + core_, "tensor": xl_ * NY + y_}

    def zat(r):
        return lax.rem(z + sgn * r + 2 * NZ, NZ)

    def yat(r):
        return lax.rem(y + sgn * r + 2 * NY, NY)

    sibling = dev(xh, z, 1 - core, xl, y)
    partner = dev(xh, z, core, 1 - xl, y)
    across = dev(1 - xh, z, core, 1 - xl, y)

    for k in range(KC):
        cols = pl.ds(k * KW, KW)
        pltpu.make_async_copy(x_hbm.at[:, cols], xw_v.at[:T, cols], lsem.at[k]).start()
        pltpu.make_async_copy(w_hbm.at[:, cols], xw_v.at[T:, cols], lsem.at[k]).start()
    x_v, w_v = xw_v.at[:T], xw_v.at[T:]
    qg_load = pltpu.make_async_copy(qg_hbm, qg_v, lsem.at[L_QG])
    qg_load.start()
    gain_load = pltpu.make_async_copy(gain_hbm, gain_v, lsem.at[L_GAIN])
    gain_load.start()
    myhalf = pl.ds(pl.multiple_of(xl * HALF, 128), HALF)
    wh_load = pltpu.make_async_copy(w_hbm.at[:, myhalf], wst_v.at[:F], lsem.at[L_WH])

    barrier = pltpu.get_barrier_semaphore()
    peers = [{"dp": d, "tensor": lax.rem(t + o, NT)} for o in range(1, NT)]
    peers += [across, sibling]
    peers += [dev(xh, zat(r), core, xl, y) for r in (1, -1, 2, -2, 4, -4)]
    peers += [dev(1 - xh, zat(r), core, xl, y) for r in (0, 1, -1, 2, -2)]
    for p in peers:
        pl.semaphore_signal(barrier, inc=1, device_id=p, device_id_type=MESH)

    pt = None
    for k in range(KC):
        cols = slice(k * KW, (k + 1) * KW)
        pltpu.make_async_copy(xw_v.at[:, cols], xw_v.at[:, cols], lsem.at[k]).wait()
        turned = x_v[:, cols].T
        h = k * KW // HALF
        for i in range(KW // 160):
            xt_v[k * KW % HALF // 160 + i, h * 160 : h * 160 + 160, :] = turned[i * 160 : i * 160 + 160]
        term = dot(w_v[:, cols], turned, ((1,), (0,)))
        pt = term if pt is None else pt + term
    wh_load.start()
    qg_load.wait()
    gain_load.wait()
    rows = lax.broadcasted_iota(jnp.int32, (F, F), 0)
    lanes = lax.broadcasted_iota(jnp.int32, (F, F), 1)
    gain = jnp.sum(jnp.where(rows == lanes, gain_v[...], 0.0), axis=1, keepdims=True)
    sg = qg_v[...].astype(F32) * gain
    sq = jnp.sum(pt * pt, axis=0, keepdims=True)
    cr = jnp.sum(sg * pt, axis=0, keepdims=True)
    sums_v[t, 0:1, :] = sq[:, :128]
    sums_v[t, 1:2, :] = sq[:, 128:]
    sums_v[t, 2:3, :] = cr[:, :128]
    sums_v[t, 3:4, :] = cr[:, 128:]

    pl.semaphore_wait(barrier, len(peers))

    def send(src, dst, ssem_at, rsem_at, device):
        pltpu.make_async_remote_copy(
            src_ref=src, dst_ref=dst, send_sem=ssem.at[ssem_at], recv_sem=rsem.at[rsem_at],
            device_id=device, device_id_type=MESH,
        ).start()

    def handle(ref, ssem_at, rsem_at):
        return pltpu.make_async_remote_copy(
            src_ref=ref, dst_ref=ref, send_sem=ssem.at[ssem_at], recv_sem=rsem.at[rsem_at],
            device_id=sibling, device_id_type=MESH,
        )

    def arrived(ref, rsem_at):
        handle(ref, 0, rsem_at).wait_recv()

    def left(ref, ssem_at):
        handle(ref, ssem_at, 0).wait_send()

    for p in peers[: NT - 1]:
        send(sums_v.at[t], sums_v.at[t], S_SUMS, SUMS, p)

    wpart = wst_v.at[F:]
    for n, who in enumerate((partner, across)):
        src = pl.ds(pl.multiple_of((1 - xl) * HALF + (2 * n + core) * CS, 128), CS)
        dst = pl.ds(pl.multiple_of((2 * n + core) * CS, 128), CS)
        send(w_v.at[:, src], wpart.at[:, dst], S_WX, WX + n, who)

    pga_v[F:, :] = jnp.zeros((256 - F, T), BF16)
    sgt_v[...] = sg.T
    ptt_v[...] = pt.T

    arrived(sums_v.at[: NT - 1], SUMS)
    total = sums_v[0]
    for s in range(1, NT):
        total = total + sums_v[s]
    sq = jnp.concatenate([total[0:1], total[1:2]], axis=1)
    cr = jnp.concatenate([total[2:3], total[3:4]], axis=1)
    inv = 1.0 / jnp.sqrt(sq / HQ + epsilon)
    coef = inv * inv * inv * (cr / HQ)
    pg = (inv * sg - coef * pt).astype(BF16)
    pga_v[:F, :] = pg
    send(pga_v.at[:F], pgp_v, S_PG, PG, partner)

    def blocks(g):
        for r in GROUPS[g]:
            v = dot(xt_v[zat(r)], pga_v[...], ((1,), (1,)))
            mirror = r if r in (0, 8) else -r
            for h in (0, 1):
                a, b = v[h * 160 : h * 160 + 80], v[h * 160 + 80 : h * 160 + 160]
                mine = packed(jnp.where(core == 0, a, b))
                other = packed(jnp.where(core == 0, b, a))
                for ref, i, parts in ((own_v, AT[r], mine), (dsend, AT[mirror], other)):
                    ref[i, h, :80, :] = parts[0].astype(ref.dtype)
                    ref[i, h, 80:96, :] = parts[1].astype(ref.dtype)
                    ref[i, h, 96:, :] = parts[2].astype(ref.dtype)
        at = pl.ds(AT[GROUPS[g][0]], len(GROUPS[g]))
        send(dsend.at[at], drecv.at[at], S_DD, DD + g, sibling)

    def local(r, h):
        return own_v[AT[r], h] + drecv[AT[r], h].astype(F32)

    def zcross(r, v):
        zs_v[AT[r], 1 - xh] = v.astype(BF16)
        send(
            zs_v.at[AT[r], 1 - xh], zrecv.at[SLOT["cross", r]], S_Z, ZC + JOINS.index(CROSS[r]),
            dev(1 - xh, zat(r - CROSS[r]), core, xl, y),
        )

    def zown(r, v):
        zs_v[AT[r], xh] = v.astype(BF16)
        send(
            zs_v.at[AT[r], xh], zrecv.at[SLOT["own", r]], S_Z, ZC + JOINS.index(PARENT[r]),
            dev(xh, zat(r - PARENT[r]), core, xl, y),
        )

    def zboth(r, pair):
        for h, v in enumerate(pair):
            zs_v[AT[r], h] = v.astype(BF16)
        send(
            zs_v.at[AT[r]], zrecv.at[pl.ds(SLOT["own", r], 2)], S_Z, ZC + JOINS.index(PARENT[r]),
            dev(xh, zat(r - PARENT[r]), core, xl, y),
        )

    def zleaf(g):
        at = pl.ds(AT[GROUPS[g][0]], len(GROUPS[g]))
        arrived(drecv.at[at], DD + g)
        for r in GROUPS[g]:
            if abs(r) >= FAR or r == 0:
                zcross(r, local(r, 1 - xh))
            if r not in JOINS:
                if abs(r) >= FAR:
                    zown(r, local(r, xh))
                else:
                    zboth(r, [local(r, h) for h in (0, 1)])

    def joined(r):
        first, n = JOIN_SLOTS[r]
        arrived(zrecv.at[pl.ds(first, n)], ZC + JOINS.index(r))
        slots = range(first, first + n)
        if abs(r) >= FAR or r == 0:
            v = local(r, xh)
            for k in slots:
                v = v + zrecv[k].astype(F32)
            return v
        pair = []
        for h in (xh, 1 - xh):
            v = local(r, h)
            for k in range(first, first + n, 2):
                v = v + zrecv[k + h].astype(F32)
            pair.append(v)
        return pair

    def zjoin(r):
        v = joined(r)
        if abs(r) >= FAR:
            zown(r, v)
        else:
            zcross(r, v[1])
            zown(r, v[0])

    def yrows(r):
        return pl.multiple_of(yat(r) * 16, 16)

    def mine(r, s, h):
        return part_v[s, pl.ds(yrows(r) + h * 128, 16), :]

    def ylast_send(slot, s, rows, dest):
        for i, who in enumerate((xl, 1 - xl)):
            if dest is None and i == 0:
                continue
            src = rows.at[pl.ds(pl.multiple_of(who * 16, 16), 16)]
            send(src, yfin.at[s, slot + i], S_YF, YF + s, dev(xh, z, core, who, y if dest is None else dest))

    def ystep(k, s):
        for r in YSTEPS[k]:
            new = [mine(r, s, h) for h in (0, 1)]
            if r not in YHEADS:
                slot = YSLOT[r]
                arrived(yrecv.at[slot, s], YC + slot * S + s)
                new = [v + yrecv[slot, s, h * 16 : h * 16 + 16, :].astype(F32) for h, v in enumerate(new)]
            to = yat(1 if r > 0 else -1)
            if abs(r) == 1:
                rows = ylast.at[0 if r > 0 else 1, s]
            else:
                slot = YSLOT[r - 1 if r > 0 else r + 1]
                rows = ysend.at[slot, s]
            for h, v in enumerate(new):
                rows[h * 16 : h * 16 + 16, :] = v.astype(BF16)
            if abs(r) == 1:
                ylast_send(0 if r > 0 else 2, s, rows, to)
            else:
                send(rows, yrecv.at[slot, s], S_Y, YC + slot * S + s, dev(xh, z, core, xl, to))

    def yown_cross(s):
        for h in (0, 1):
            ylast[2, s, h * 16 : h * 16 + 16, :] = mine(0, s, h).astype(BF16)
        ylast_send(3, s, ylast.at[2, s], None)

    blocks(0)
    for n in (0, 1):
        cols = pl.ds(pl.multiple_of((2 * n + core) * CS, 128), CS)
        arrived(wpart.at[:, cols], WX + n)
        send(wpart.at[:, cols], wpart.at[:, cols], S_WD, WD + n, sibling)
    wh_load.wait()
    blocks(1)
    zleaf(0)
    both = jnp.concatenate([inv, coef], axis=0)
    both = jnp.concatenate([both, jnp.zeros((6, T), F32)], axis=0).T
    own = (both[:, 0:1] * sgt_v[...] - both[:, 1:2] * ptt_v[...]).astype(BF16)
    for s in range(S):
        part_v[s] = dot(own, wst_v[:F, s * CS : (s + 1) * CS], ((1,), (0,)))
    zleaf(1)
    arrived(pgp_v, PG)
    for n in (0, 1):
        cols = pl.ds(pl.multiple_of((2 * n + 1 - core) * CS, 128), CS)
        arrived(wpart.at[:, cols], WD + n)
    for s in range(S):
        part_v[s] += dot(pgp_v[...], wst_v[F:, s * CS : (s + 1) * CS], ((0,), (0,)))
        ystep(0, s)
    for s in range(S):
        yown_cross(s)
    blocks(2)
    blocks(3)
    zleaf(2)
    zleaf(3)
    for s in (0, 1):
        ystep(1, s)
    for s in (2, 3):
        ystep(1, s)
    zjoin(6)
    zjoin(-6)
    for s in (0, 1):
        ystep(2, s)
    for s in (2, 3):
        ystep(2, s)
    zjoin(1)
    zjoin(-1)
    zjoin(4)
    zjoin(-4)
    for s in (0, 1):
        ystep(3, s)
    for s in (2, 3):
        ystep(3, s)
    for s in range(S):
        arrived(yfin.at[s], YF + s)
        own = part_v[s, pl.ds(yrows(0) + xl * 128, 16), :]
        for who, v, slots in ((xl, own, (0, 2)), (1 - xl, 0.0, (1, 3, 4))):
            for slot in slots:
                v = v + yfin[s, slot].astype(F32)
            cols = pl.ds(pl.multiple_of(who * HALF + s * CS, 128), CS)
            out_v[:, cols] = v.astype(BF16)

    v = joined(0)
    wg_v[:, :128] = v[:80]
    wg_v[:16, 128:] = v[80:96, :32]
    for j in (1, 2, 3):
        wg_v[16 * j : 16 * j + 16, 128:] = pltpu.roll(v[80:96], 128 - 32 * j, 1)[:, :32]
    wg_v[64:, 128:] = v[96:, :32]

    left(sums_v.at[: NT - 1], S_SUMS)
    left(wpart.at[:, : 2 * CS], S_WX)
    left(wpart.at[:, : 2 * CS], S_WD)
    left(pgp_v, S_PG)
    left(dsend, S_DD)
    left(zrecv, S_Z)
    left(yrecv, S_Y)
    left(yfin, S_YF)


def per_device(block_input, query_weight, query_gain, query_grad):
    hbm = pl.BlockSpec(memory_space=pltpu.HBM)
    vmem = pl.BlockSpec(memory_space=pltpu.VMEM)
    outs = (jax.ShapeDtypeStruct((T // NT, D), BF16), jax.ShapeDtypeStruct((80, F), F32))
    return pl.pallas_call(
        kernel,
        out_shape=outs,
        in_specs=[hbm, hbm, hbm, hbm],
        out_specs=(vmem, vmem),
        scratch_shapes=[
            pltpu.VMEM((T + F, D), BF16),
            pltpu.VMEM((NZ, 320, T), BF16),
            pltpu.VMEM((2 * F, HALF), BF16),
            pltpu.VMEM((1, F), F32),
            pltpu.VMEM((F, T), BF16),
            pltpu.VMEM((NT, 4, 128), F32),
            pltpu.VMEM((256, T), BF16),
            pltpu.VMEM((F, T), BF16),
            pltpu.VMEM((T, F), F32),
            pltpu.VMEM((T, F), F32),
            pltpu.VMEM((16, 2, PACK, 128), BF16),
            pltpu.VMEM((16, 2, PACK, 128), BF16),
            pltpu.VMEM((16, 2, PACK, 128), F32),
            pltpu.VMEM((16, 2, PACK, 128), BF16),
            pltpu.VMEM((NSLOT, PACK, 128), BF16),
            pltpu.VMEM((S, T, CS), F32),
            pltpu.VMEM((5, S, 32, CS), BF16),
            pltpu.VMEM((5, S, 32, CS), BF16),
            pltpu.VMEM((3, S, 32, CS), BF16),
            pltpu.VMEM((S, 5, 16, CS), BF16),
            pltpu.SemaphoreType.DMA((KC + 3,)),
            pltpu.SemaphoreType.DMA((8,)),
            pltpu.SemaphoreType.DMA((NRECV,)),
        ],
        compiler_params=pltpu.CompilerParams(
            collective_id=0, has_side_effects=True, vmem_limit_bytes=40 * 1024 * 1024
        ),
    )(*(pltpu.with_memory_space_constraint(a, pltpu.HBM) for a in (block_input, query_weight, query_gain.reshape(1, F), query_grad)))


def solution(mesh):
    return jax.shard_map(
        per_device,
        mesh=mesh,
        in_specs=(P("dp", None), P("tensor", None), P("tensor"), P("tensor", "dp")),
        out_specs=(P(("dp", "tensor"), None), P("dp", "tensor")),
        check_vma=False,
    )
```

```python
import jax
import jax.numpy as jnp
from jax import lax
from jax.experimental import pallas as pl
from jax.experimental.pallas import tpu as pltpu
from jax.sharding import PartitionSpec as P

MESH = pl.DeviceIdType.MESH
F32, BF16 = jnp.float32, jnp.bfloat16

NT, NY, NZ = 16, 8, 16
T, F, D = 256, 160, 5120
HALF = D // 2
S = 5
CS = HALF // S
WS = HALF // 4
KC = 8
KW = D // KC
HQ = F * NT
epsilon = 1e-6

PARENT = {8: 6, 7: 6, 6: 4, 5: 4, 4: 0, 3: 1, 2: 1, 1: 0, -7: -6, -6: -4, -5: -4, -4: 0, -3: -1, -2: -1, -1: 0}
CROSS = {8: 6, 7: 6, 6: 6, 5: 4, 4: 4, -7: -6, -6: -6, -5: -4, -4: -4, 1: 0, -1: 0, 0: 0}
GROUPS = ((8, 7, -7), (6, -6, 5, -5), (4, -4, 3, -3), (2, -2, 1, -1, 0))
ORDER = sum(GROUPS, ())
AT = {r: i for i, r in enumerate(ORDER)}
JOINS = (6, -6, 4, -4, 1, -1, 0)
FAR = 4
SLOT, JOIN_SLOTS = {}, {}
count = 0
for j in JOINS:
    first = count
    for r in ORDER:
        if PARENT.get(r) == j:
            SLOT["own", r] = count
            count += 2 if abs(r) < FAR and j else 1
        if CROSS.get(r) == j:
            SLOT["cross", r] = count
            count += 1
    JOIN_SLOTS[j] = (first, count - first)
NSLOT = count
PACK = 112

YSTEPS = ((4, -3), (3, -2), (2, -1), (1,))
YHEADS = (4, -3)
YSLOT = {3: 0, 2: 1, 1: 2, -2: 3, -1: 4}

SUMS, WX, WD, PG = 0, 1, 3, 5
DD = 6
ZC = DD + len(GROUPS)
YC = ZC + len(JOINS)
YF = YC + 5 * S
NRECV = YF + S
S_SUMS, S_WX, S_WD, S_PG, S_DD, S_Z, S_Y, S_YF = range(8)
L_QG, L_GAIN, L_WH = KC, KC + 1, KC + 2


def dot(a, b, dims):
    return lax.dot_general(a, b, (dims, ((), ())), preferred_element_type=F32)


def packed(v):
    rest = v[:, 128:]
    tile = rest[:16]
    for j in (1, 2, 3):
        tile = tile + pltpu.roll(rest[16 * j : 16 * j + 16], 32 * j, 1)
    return v[:, :128], tile, rest[64:]


def kernel(
    x_hbm, w_hbm, gain_hbm, qg_hbm, out_v, wg_v,
    xw_v, xt_v, wst_v, gain_v, qg_v, sums_v, pga_v, pgp_v, sgt_v, ptt_v,
    dsend, drecv, own_v, zs_v, zrecv,
    part_v, ysend, yrecv, ylast, yfin,
    lsem, ssem, rsem,
):
    d = lax.axis_index("dp")
    t = lax.axis_index("tensor")
    core = lax.rem(d, 2)
    z = lax.rem(lax.div(d, 2), NZ)
    xh = lax.div(d, 2 * NZ)
    y = lax.rem(t, NY)
    xl = lax.div(t, NY)
    sgn = 1 - 2 * core

    def dev(xh_, z_, core_, xl_, y_):
        return {"dp": (xh_ * NZ + z_) * 2 + core_, "tensor": xl_ * NY + y_}

    def zat(r):
        return lax.rem(z + sgn * r + 2 * NZ, NZ)

    def yat(r):
        return lax.rem(y + sgn * r + 2 * NY, NY)

    sibling = dev(xh, z, 1 - core, xl, y)
    partner = dev(xh, z, core, 1 - xl, y)
    across = dev(1 - xh, z, core, 1 - xl, y)

    for k in range(KC):
        cols = pl.ds(k * KW, KW)
        pltpu.make_async_copy(x_hbm.at[:, cols], xw_v.at[:T, cols], lsem.at[k]).start()
        pltpu.make_async_copy(w_hbm.at[:, cols], xw_v.at[T:, cols], lsem.at[k]).start()
    x_v, w_v = xw_v.at[:T], xw_v.at[T:]
    qg_load = pltpu.make_async_copy(qg_hbm, qg_v, lsem.at[L_QG])
    qg_load.start()
    gain_load = pltpu.make_async_copy(gain_hbm, gain_v, lsem.at[L_GAIN])
    gain_load.start()
    myhalf = pl.ds(pl.multiple_of(xl * HALF, 128), HALF)
    wh_load = pltpu.make_async_copy(w_hbm.at[:, myhalf], wst_v.at[:F], lsem.at[L_WH])

    barrier = pltpu.get_barrier_semaphore()
    peers = [{"dp": d, "tensor": lax.rem(t + o, NT)} for o in range(1, NT)]
    peers += [across, sibling]
    peers += [dev(xh, zat(r), core, xl, y) for r in (1, -1, 2, -2, 4, -4)]
    peers += [dev(1 - xh, zat(r), core, xl, y) for r in (0, 1, -1, 2, -2)]
    for p in peers:
        pl.semaphore_signal(barrier, inc=1, device_id=p, device_id_type=MESH)

    pt = None
    for k in range(KC):
        cols = slice(k * KW, (k + 1) * KW)
        pltpu.make_async_copy(xw_v.at[:, cols], xw_v.at[:, cols], lsem.at[k]).wait()
        turned = x_v[:, cols].T
        h = k * KW // HALF
        for i in range(KW // 160):
            xt_v[k * KW % HALF // 160 + i, h * 160 : h * 160 + 160, :] = turned[i * 160 : i * 160 + 160]
        term = dot(w_v[:, cols], turned, ((1,), (0,)))
        pt = term if pt is None else pt + term
    wh_load.start()
    qg_load.wait()
    gain_load.wait()
    rows = lax.broadcasted_iota(jnp.int32, (F, F), 0)
    lanes = lax.broadcasted_iota(jnp.int32, (F, F), 1)
    gain = jnp.sum(jnp.where(rows == lanes, gain_v[...], 0.0), axis=1, keepdims=True)
    sg = qg_v[...].astype(F32) * gain
    sq = jnp.sum(pt * pt, axis=0, keepdims=True)
    cr = jnp.sum(sg * pt, axis=0, keepdims=True)
    sums_v[t, 0:1, :] = sq[:, :128]
    sums_v[t, 1:2, :] = sq[:, 128:]
    sums_v[t, 2:3, :] = cr[:, :128]
    sums_v[t, 3:4, :] = cr[:, 128:]

    pl.semaphore_wait(barrier, len(peers))

    def send(src, dst, ssem_at, rsem_at, device):
        pltpu.make_async_remote_copy(
            src_ref=src, dst_ref=dst, send_sem=ssem.at[ssem_at], recv_sem=rsem.at[rsem_at],
            device_id=device, device_id_type=MESH,
        ).start()

    def handle(ref, ssem_at, rsem_at):
        return pltpu.make_async_remote_copy(
            src_ref=ref, dst_ref=ref, send_sem=ssem.at[ssem_at], recv_sem=rsem.at[rsem_at],
            device_id=sibling, device_id_type=MESH,
        )

    def arrived(ref, rsem_at):
        handle(ref, 0, rsem_at).wait_recv()

    def left(ref, ssem_at):
        handle(ref, ssem_at, 0).wait_send()

    for p in peers[: NT - 1]:
        send(sums_v.at[t], sums_v.at[t], S_SUMS, SUMS, p)

    wpart = wst_v.at[F:]
    for n, who in enumerate((partner, across)):
        src = pl.ds(pl.multiple_of((1 - xl) * HALF + (2 * n + core) * WS, 128), WS)
        dst = pl.ds(pl.multiple_of((2 * n + core) * WS, 128), WS)
        send(w_v.at[:, src], wpart.at[:, dst], S_WX, WX + n, who)

    pga_v[F:, :] = jnp.zeros((256 - F, T), BF16)
    sgt_v[...] = sg.T
    ptt_v[...] = pt.T

    arrived(sums_v.at[: NT - 1], SUMS)
    total = sums_v[0]
    for s in range(1, NT):
        total = total + sums_v[s]
    sq = jnp.concatenate([total[0:1], total[1:2]], axis=1)
    cr = jnp.concatenate([total[2:3], total[3:4]], axis=1)
    inv = 1.0 / jnp.sqrt(sq / HQ + epsilon)
    coef = inv * inv * inv * (cr / HQ)
    pg = (inv * sg - coef * pt).astype(BF16)
    pga_v[:F, :] = pg
    send(pga_v.at[:F], pgp_v, S_PG, PG, partner)

    def blocks(g):
        for r in GROUPS[g]:
            v = dot(xt_v[zat(r)], pga_v[...], ((1,), (1,)))
            mirror = r if r in (0, 8) else -r
            for h in (0, 1):
                a, b = v[h * 160 : h * 160 + 80], v[h * 160 + 80 : h * 160 + 160]
                mine = packed(jnp.where(core == 0, a, b))
                other = packed(jnp.where(core == 0, b, a))
                for ref, i, parts in ((own_v, AT[r], mine), (dsend, AT[mirror], other)):
                    ref[i, h, :80, :] = parts[0].astype(ref.dtype)
                    ref[i, h, 80:96, :] = parts[1].astype(ref.dtype)
                    ref[i, h, 96:, :] = parts[2].astype(ref.dtype)
        at = pl.ds(AT[GROUPS[g][0]], len(GROUPS[g]))
        send(dsend.at[at], drecv.at[at], S_DD, DD + g, sibling)

    def local(r, h):
        return own_v[AT[r], h] + drecv[AT[r], h].astype(F32)

    def zcross(r, v):
        zs_v[AT[r], 1 - xh] = v.astype(BF16)
        send(
            zs_v.at[AT[r], 1 - xh], zrecv.at[SLOT["cross", r]], S_Z, ZC + JOINS.index(CROSS[r]),
            dev(1 - xh, zat(r - CROSS[r]), core, xl, y),
        )

    def zown(r, v):
        zs_v[AT[r], xh] = v.astype(BF16)
        send(
            zs_v.at[AT[r], xh], zrecv.at[SLOT["own", r]], S_Z, ZC + JOINS.index(PARENT[r]),
            dev(xh, zat(r - PARENT[r]), core, xl, y),
        )

    def zboth(r, pair):
        for h, v in enumerate(pair):
            zs_v[AT[r], h] = v.astype(BF16)
        send(
            zs_v.at[AT[r]], zrecv.at[pl.ds(SLOT["own", r], 2)], S_Z, ZC + JOINS.index(PARENT[r]),
            dev(xh, zat(r - PARENT[r]), core, xl, y),
        )

    def zleaf(g):
        at = pl.ds(AT[GROUPS[g][0]], len(GROUPS[g]))
        arrived(drecv.at[at], DD + g)
        for r in GROUPS[g]:
            if abs(r) >= FAR or r == 0:
                zcross(r, local(r, 1 - xh))
            if r not in JOINS:
                if abs(r) >= FAR:
                    zown(r, local(r, xh))
                else:
                    zboth(r, [local(r, h) for h in (0, 1)])

    def joined(r):
        first, n = JOIN_SLOTS[r]
        arrived(zrecv.at[pl.ds(first, n)], ZC + JOINS.index(r))
        slots = range(first, first + n)
        if abs(r) >= FAR or r == 0:
            v = local(r, xh)
            for k in slots:
                v = v + zrecv[k].astype(F32)
            return v
        pair = []
        for h in (xh, 1 - xh):
            v = local(r, h)
            for k in range(first, first + n, 2):
                v = v + zrecv[k + h].astype(F32)
            pair.append(v)
        return pair

    def zjoin(r):
        v = joined(r)
        if abs(r) >= FAR:
            zown(r, v)
        else:
            zcross(r, v[1])
            zown(r, v[0])

    def yrows(r):
        return pl.multiple_of(yat(r) * 16, 16)

    def mine(r, s, h):
        return part_v[s, pl.ds(yrows(r) + h * 128, 16), :]

    def ylast_send(slot, s, rows, dest):
        for i, who in enumerate((xl, 1 - xl)):
            if dest is None and i == 0:
                continue
            src = rows.at[pl.ds(pl.multiple_of(who * 16, 16), 16)]
            send(src, yfin.at[s, slot + i], S_YF, YF + s, dev(xh, z, core, who, y if dest is None else dest))

    def ystep(k, s):
        for r in YSTEPS[k]:
            new = [mine(r, s, h) for h in (0, 1)]
            if r not in YHEADS:
                slot = YSLOT[r]
                arrived(yrecv.at[slot, s], YC + slot * S + s)
                new = [v + yrecv[slot, s, h * 16 : h * 16 + 16, :].astype(F32) for h, v in enumerate(new)]
            to = yat(1 if r > 0 else -1)
            if abs(r) == 1:
                rows = ylast.at[0 if r > 0 else 1, s]
            else:
                slot = YSLOT[r - 1 if r > 0 else r + 1]
                rows = ysend.at[slot, s]
            for h, v in enumerate(new):
                rows[h * 16 : h * 16 + 16, :] = v.astype(BF16)
            if abs(r) == 1:
                ylast_send(0 if r > 0 else 2, s, rows, to)
            else:
                send(rows, yrecv.at[slot, s], S_Y, YC + slot * S + s, dev(xh, z, core, xl, to))

    def yown_cross(s):
        for h in (0, 1):
            ylast[2, s, h * 16 : h * 16 + 16, :] = mine(0, s, h).astype(BF16)
        ylast_send(3, s, ylast.at[2, s], None)

    blocks(0)
    for n in (0, 1):
        cols = pl.ds(pl.multiple_of((2 * n + core) * WS, 128), WS)
        arrived(wpart.at[:, cols], WX + n)
        send(wpart.at[:, cols], wpart.at[:, cols], S_WD, WD + n, sibling)
    wh_load.wait()
    blocks(1)
    zleaf(0)
    both = jnp.concatenate([inv, coef], axis=0)
    both = jnp.concatenate([both, jnp.zeros((6, T), F32)], axis=0).T
    own = (both[:, 0:1] * sgt_v[...] - both[:, 1:2] * ptt_v[...]).astype(BF16)
    for s in range(S):
        part_v[s] = dot(own, wst_v[:F, s * CS : (s + 1) * CS], ((1,), (0,)))
    zleaf(1)
    arrived(pgp_v, PG)
    for n in (0, 1):
        cols = pl.ds(pl.multiple_of((2 * n + 1 - core) * WS, 128), WS)
        arrived(wpart.at[:, cols], WD + n)
    for s in range(S):
        part_v[s] += dot(pgp_v[...], wst_v[F:, s * CS : (s + 1) * CS], ((0,), (0,)))
        ystep(0, s)
    for s in range(S):
        yown_cross(s)
    blocks(2)
    blocks(3)
    zleaf(2)
    zleaf(3)
    for s in (0, 1):
        ystep(1, s)
    for s in (2, 3, 4):
        ystep(1, s)
    zjoin(6)
    zjoin(-6)
    for s in (0, 1):
        ystep(2, s)
    for s in (2, 3, 4):
        ystep(2, s)
    zjoin(1)
    zjoin(-1)
    zjoin(4)
    zjoin(-4)
    for s in (0, 1):
        ystep(3, s)
    for s in (2, 3, 4):
        ystep(3, s)
    for s in range(S):
        arrived(yfin.at[s], YF + s)
        own = part_v[s, pl.ds(yrows(0) + xl * 128, 16), :]
        for who, v, slots in ((xl, own, (0, 2)), (1 - xl, 0.0, (1, 3, 4))):
            for slot in slots:
                v = v + yfin[s, slot].astype(F32)
            cols = pl.ds(pl.multiple_of(who * HALF + s * CS, 128), CS)
            out_v[:, cols] = v.astype(BF16)

    v = joined(0)
    wg_v[:, :128] = v[:80]
    wg_v[:16, 128:] = v[80:96, :32]
    for j in (1, 2, 3):
        wg_v[16 * j : 16 * j + 16, 128:] = pltpu.roll(v[80:96], 128 - 32 * j, 1)[:, :32]
    wg_v[64:, 128:] = v[96:, :32]

    left(sums_v.at[: NT - 1], S_SUMS)
    left(wpart.at[:, : 2 * WS], S_WX)
    left(wpart.at[:, : 2 * WS], S_WD)
    left(pgp_v, S_PG)
    left(dsend, S_DD)
    left(zrecv, S_Z)
    left(yrecv, S_Y)
    left(yfin, S_YF)


def per_device(block_input, query_weight, query_gain, query_grad):
    hbm = pl.BlockSpec(memory_space=pltpu.HBM)
    vmem = pl.BlockSpec(memory_space=pltpu.VMEM)
    outs = (jax.ShapeDtypeStruct((T // NT, D), BF16), jax.ShapeDtypeStruct((80, F), F32))
    return pl.pallas_call(
        kernel,
        out_shape=outs,
        in_specs=[hbm, hbm, hbm, hbm],
        out_specs=(vmem, vmem),
        scratch_shapes=[
            pltpu.VMEM((T + F, D), BF16),
            pltpu.VMEM((NZ, 320, T), BF16),
            pltpu.VMEM((2 * F, HALF), BF16),
            pltpu.VMEM((1, F), F32),
            pltpu.VMEM((F, T), BF16),
            pltpu.VMEM((NT, 4, 128), F32),
            pltpu.VMEM((256, T), BF16),
            pltpu.VMEM((F, T), BF16),
            pltpu.VMEM((T, F), F32),
            pltpu.VMEM((T, F), F32),
            pltpu.VMEM((16, 2, PACK, 128), BF16),
            pltpu.VMEM((16, 2, PACK, 128), BF16),
            pltpu.VMEM((16, 2, PACK, 128), F32),
            pltpu.VMEM((16, 2, PACK, 128), BF16),
            pltpu.VMEM((NSLOT, PACK, 128), BF16),
            pltpu.VMEM((S, T, CS), F32),
            pltpu.VMEM((5, S, 32, CS), BF16),
            pltpu.VMEM((5, S, 32, CS), BF16),
            pltpu.VMEM((3, S, 32, CS), BF16),
            pltpu.VMEM((S, 5, 16, CS), BF16),
            pltpu.SemaphoreType.DMA((KC + 3,)),
            pltpu.SemaphoreType.DMA((8,)),
            pltpu.SemaphoreType.DMA((NRECV,)),
        ],
        compiler_params=pltpu.CompilerParams(
            collective_id=0, has_side_effects=True, vmem_limit_bytes=40 * 1024 * 1024
        ),
    )(*(pltpu.with_memory_space_constraint(a, pltpu.HBM) for a in (block_input, query_weight, query_gain.reshape(1, F), query_grad)))


def solution(mesh):
    return jax.shard_map(
        per_device,
        mesh=mesh,
        in_specs=(P("dp", None), P("tensor", None), P("tensor"), P("tensor", "dp")),
        out_specs=(P(("dp", "tensor"), None), P("dp", "tensor")),
        check_vma=False,
    )
```

```python
import jax
import jax.numpy as jnp
from jax import lax
from jax.experimental import pallas as pl
from jax.experimental.pallas import tpu as pltpu
from jax.sharding import PartitionSpec as P

MESH = pl.DeviceIdType.MESH
F32, BF16 = jnp.float32, jnp.bfloat16

NT, NY, NZ = 16, 8, 16
T, F, D = 256, 160, 5120
HALF = D // 2
S = 4
CS = HALF // S
KC = 8
KW = D // KC
HQ = F * NT
epsilon = 1e-6

PARENT = {8: 6, 7: 6, 6: 4, 5: 4, 4: 0, 3: 1, 2: 1, 1: 0, -7: -6, -6: -4, -5: -4, -4: 0, -3: -1, -2: -1, -1: 0}
CROSS = {8: 6, 7: 6, 6: 6, 5: 4, 4: 4, -7: -6, -6: -6, -5: -4, -4: -4, 1: 0, -1: 0, 0: 0}
GROUPS = ((8, 7, -7), (6, -6, 5, -5), (4, -4, 3, -3), (2, -2, 1, -1, 0))
ORDER = sum(GROUPS, ())
AT = {r: i for i, r in enumerate(ORDER)}
JOINS = (6, -6, 4, -4, 1, -1, 0)
FAR = 4
SLOT, JOIN_SLOTS = {}, {}
count = 0
for j in JOINS:
    first = count
    for r in ORDER:
        if PARENT.get(r) == j:
            SLOT["own", r] = count
            count += 2 if abs(r) < FAR and j else 1
        if CROSS.get(r) == j:
            SLOT["cross", r] = count
            count += 1
    JOIN_SLOTS[j] = (first, count - first)
NSLOT = count
PACK = 112

YSTEPS = ((4, -3), (3, -2), (2, -1), (1,))
YHEADS = (4, -3)
YSLOT = {3: 0, 2: 1, 1: 2, -2: 3, -1: 4}

SUMS, WX, WD, PG = 0, 1, 3, 5
DD = 6
ZC = DD + len(GROUPS)
YC = ZC + len(JOINS)
YF = YC + 5 * S
NRECV = YF + S
S_SUMS, S_WX, S_WD, S_PG, S_DD, S_Z, S_Y, S_YF = range(8)
L_QG, L_GAIN, L_WH = KC, KC + 1, KC + 2


def dot(a, b, dims):
    return lax.dot_general(a, b, (dims, ((), ())), preferred_element_type=F32)


def packed(v):
    rest = v[:, 128:]
    tile = rest[:16]
    for j in (1, 2, 3):
        tile = tile + pltpu.roll(rest[16 * j : 16 * j + 16], 32 * j, 1)
    return v[:, :128], tile, rest[64:]


def kernel(
    x_hbm, w_hbm, gain_hbm, qg_hbm, out_v, wg_v,
    xw_v, xt_v, wst_v, gain_v, qg_v, sums_v, pga_v, pgp_v, sgt_v, ptt_v,
    dsend, drecv, own_v, zs_v, zrecv,
    part_v, ysend, yrecv, ylast, yfin,
    lsem, ssem, rsem,
):
    d = lax.axis_index("dp")
    t = lax.axis_index("tensor")
    core = lax.rem(d, 2)
    z = lax.rem(lax.div(d, 2), NZ)
    xh = lax.div(d, 2 * NZ)
    y = lax.rem(t, NY)
    xl = lax.div(t, NY)
    sgn = 1 - 2 * core

    def dev(xh_, z_, core_, xl_, y_):
        return {"dp": (xh_ * NZ + z_) * 2 + core_, "tensor": xl_ * NY + y_}

    def zat(r):
        return lax.rem(z + sgn * r + 2 * NZ, NZ)

    def yat(r):
        return lax.rem(y + sgn * r + 2 * NY, NY)

    sibling = dev(xh, z, 1 - core, xl, y)
    partner = dev(xh, z, core, 1 - xl, y)
    across = dev(1 - xh, z, core, 1 - xl, y)

    for k in range(KC):
        cols = pl.ds(k * KW, KW)
        pltpu.make_async_copy(x_hbm.at[:, cols], xw_v.at[:T, cols], lsem.at[k]).start()
        pltpu.make_async_copy(w_hbm.at[:, cols], xw_v.at[T:, cols], lsem.at[k]).start()
    x_v, w_v = xw_v.at[:T], xw_v.at[T:]
    qg_load = pltpu.make_async_copy(qg_hbm, qg_v, lsem.at[L_QG])
    qg_load.start()
    gain_load = pltpu.make_async_copy(gain_hbm, gain_v, lsem.at[L_GAIN])
    gain_load.start()
    myhalf = pl.ds(pl.multiple_of(xl * HALF, 128), HALF)
    wh_load = pltpu.make_async_copy(w_hbm.at[:, myhalf], wst_v.at[:F], lsem.at[L_WH])

    barrier = pltpu.get_barrier_semaphore()
    peers = [{"dp": d, "tensor": lax.rem(t + o, NT)} for o in range(1, NT)]
    peers += [across, sibling]
    peers += [dev(xh, zat(r), core, xl, y) for r in (1, -1, 2, -2, 4, -4)]
    peers += [dev(1 - xh, zat(r), core, xl, y) for r in (0, 1, -1, 2, -2)]
    for p in peers:
        pl.semaphore_signal(barrier, inc=1, device_id=p, device_id_type=MESH)

    pt = None
    for k in range(KC):
        cols = slice(k * KW, (k + 1) * KW)
        pltpu.make_async_copy(xw_v.at[:, cols], xw_v.at[:, cols], lsem.at[k]).wait()
        turned = x_v[:, cols].T
        h = k * KW // HALF
        for i in range(KW // 160):
            xt_v[k * KW % HALF // 160 + i, h * 160 : h * 160 + 160, :] = turned[i * 160 : i * 160 + 160]
        term = dot(w_v[:, cols], turned, ((1,), (0,)))
        pt = term if pt is None else pt + term
    wh_load.start()
    qg_load.wait()
    gain_load.wait()
    rows = lax.broadcasted_iota(jnp.int32, (F, F), 0)
    lanes = lax.broadcasted_iota(jnp.int32, (F, F), 1)
    gain = jnp.sum(jnp.where(rows == lanes, gain_v[...], 0.0), axis=1, keepdims=True)
    sg = qg_v[...].astype(F32) * gain
    sq = jnp.sum(pt * pt, axis=0, keepdims=True)
    cr = jnp.sum(sg * pt, axis=0, keepdims=True)
    sums_v[t, 0:1, :] = sq[:, :128]
    sums_v[t, 1:2, :] = sq[:, 128:]
    sums_v[t, 2:3, :] = cr[:, :128]
    sums_v[t, 3:4, :] = cr[:, 128:]

    pl.semaphore_wait(barrier, len(peers))

    def send(src, dst, ssem_at, rsem_at, device):
        pltpu.make_async_remote_copy(
            src_ref=src, dst_ref=dst, send_sem=ssem.at[ssem_at], recv_sem=rsem.at[rsem_at],
            device_id=device, device_id_type=MESH,
        ).start()

    def handle(ref, ssem_at, rsem_at):
        return pltpu.make_async_remote_copy(
            src_ref=ref, dst_ref=ref, send_sem=ssem.at[ssem_at], recv_sem=rsem.at[rsem_at],
            device_id=sibling, device_id_type=MESH,
        )

    def arrived(ref, rsem_at):
        handle(ref, 0, rsem_at).wait_recv()

    def left(ref, ssem_at):
        handle(ref, ssem_at, 0).wait_send()

    for p in peers[: NT - 1]:
        send(sums_v.at[t], sums_v.at[t], S_SUMS, SUMS, p)

    wpart = wst_v.at[F:]
    for n, who in enumerate((partner, across)):
        src = pl.ds(pl.multiple_of((1 - xl) * HALF + (2 * n + core) * CS, 128), CS)
        dst = pl.ds(pl.multiple_of((2 * n + core) * CS, 128), CS)
        send(w_v.at[:, src], wpart.at[:, dst], S_WX, WX + n, who)

    pga_v[F:, :] = jnp.zeros((256 - F, T), BF16)
    sgt_v[...] = sg.T
    ptt_v[...] = pt.T

    arrived(sums_v.at[: NT - 1], SUMS)
    total = sums_v[0]
    for s in range(1, NT):
        total = total + sums_v[s]
    sq = jnp.concatenate([total[0:1], total[1:2]], axis=1)
    cr = jnp.concatenate([total[2:3], total[3:4]], axis=1)
    inv = 1.0 / jnp.sqrt(sq / HQ + epsilon)
    coef = inv * inv * inv * (cr / HQ)
    pg = (inv * sg - coef * pt).astype(BF16)
    pga_v[:F, :] = pg
    send(pga_v.at[:F], pgp_v, S_PG, PG, partner)

    def blocks(g):
        for r in GROUPS[g]:
            v = dot(xt_v[zat(r)], pga_v[...], ((1,), (1,)))
            mirror = r if r in (0, 8) else -r
            for h in (0, 1):
                a, b = v[h * 160 : h * 160 + 80], v[h * 160 + 80 : h * 160 + 160]
                mine = packed(jnp.where(core == 0, a, b))
                other = packed(jnp.where(core == 0, b, a))
                for ref, i, parts in ((own_v, AT[r], mine), (dsend, AT[mirror], other)):
                    ref[i, h, :80, :] = parts[0].astype(ref.dtype)
                    ref[i, h, 80:96, :] = parts[1].astype(ref.dtype)
                    ref[i, h, 96:, :] = parts[2].astype(ref.dtype)
        at = pl.ds(AT[GROUPS[g][0]], len(GROUPS[g]))
        send(dsend.at[at], drecv.at[at], S_DD, DD + g, sibling)

    def local(r, h):
        return own_v[AT[r], h] + drecv[AT[r], h].astype(F32)

    def zcross(r, v):
        zs_v[AT[r], 1 - xh] = v.astype(BF16)
        send(
            zs_v.at[AT[r], 1 - xh], zrecv.at[SLOT["cross", r]], S_Z, ZC + JOINS.index(CROSS[r]),
            dev(1 - xh, zat(r - CROSS[r]), core, xl, y),
        )

    def zown(r, v):
        zs_v[AT[r], xh] = v.astype(BF16)
        send(
            zs_v.at[AT[r], xh], zrecv.at[SLOT["own", r]], S_Z, ZC + JOINS.index(PARENT[r]),
            dev(xh, zat(r - PARENT[r]), core, xl, y),
        )

    def zboth(r, pair):
        for h, v in enumerate(pair):
            zs_v[AT[r], h] = v.astype(BF16)
        send(
            zs_v.at[AT[r]], zrecv.at[pl.ds(SLOT["own", r], 2)], S_Z, ZC + JOINS.index(PARENT[r]),
            dev(xh, zat(r - PARENT[r]), core, xl, y),
        )

    def zleaf(g):
        at = pl.ds(AT[GROUPS[g][0]], len(GROUPS[g]))
        arrived(drecv.at[at], DD + g)
        for r in GROUPS[g]:
            if abs(r) >= FAR or r == 0:
                zcross(r, local(r, 1 - xh))
            if r not in JOINS:
                if abs(r) >= FAR:
                    zown(r, local(r, xh))
                else:
                    zboth(r, [local(r, h) for h in (0, 1)])

    def joined(r):
        first, n = JOIN_SLOTS[r]
        arrived(zrecv.at[pl.ds(first, n)], ZC + JOINS.index(r))
        slots = range(first, first + n)
        if abs(r) >= FAR or r == 0:
            v = local(r, xh)
            for k in slots:
                v = v + zrecv[k].astype(F32)
            return v
        pair = []
        for h in (xh, 1 - xh):
            v = local(r, h)
            for k in range(first, first + n, 2):
                v = v + zrecv[k + h].astype(F32)
            pair.append(v)
        return pair

    def zjoin(r):
        v = joined(r)
        if abs(r) >= FAR:
            zown(r, v)
        else:
            zcross(r, v[1])
            zown(r, v[0])

    def yrows(r):
        return pl.multiple_of(yat(r) * 16, 16)

    def mine(r, s, h):
        return part_v[s, pl.ds(yrows(r) + h * 128, 16), :]

    def ylast_send(slot, s, rows, dest):
        for i, who in enumerate((xl, 1 - xl)):
            if dest is None and i == 0:
                continue
            src = rows.at[pl.ds(pl.multiple_of(who * 16, 16), 16)]
            send(src, yfin.at[s, slot + i], S_YF, YF + s, dev(xh, z, core, who, y if dest is None else dest))

    def ystep(k, s):
        for r in YSTEPS[k]:
            new = [mine(r, s, h) for h in (0, 1)]
            if r not in YHEADS:
                slot = YSLOT[r]
                arrived(yrecv.at[slot, s], YC + slot * S + s)
                new = [v + yrecv[slot, s, h * 16 : h * 16 + 16, :].astype(F32) for h, v in enumerate(new)]
            to = yat(1 if r > 0 else -1)
            if abs(r) == 1:
                rows = ylast.at[0 if r > 0 else 1, s]
            else:
                slot = YSLOT[r - 1 if r > 0 else r + 1]
                rows = ysend.at[slot, s]
            for h, v in enumerate(new):
                rows[h * 16 : h * 16 + 16, :] = v.astype(BF16)
            if abs(r) == 1:
                ylast_send(0 if r > 0 else 2, s, rows, to)
            else:
                send(rows, yrecv.at[slot, s], S_Y, YC + slot * S + s, dev(xh, z, core, xl, to))

    def yown_cross(s):
        for h in (0, 1):
            ylast[2, s, h * 16 : h * 16 + 16, :] = mine(0, s, h).astype(BF16)
        ylast_send(3, s, ylast.at[2, s], None)

    blocks(0)
    for n in (0, 1):
        cols = pl.ds(pl.multiple_of((2 * n + core) * CS, 128), CS)
        arrived(wpart.at[:, cols], WX + n)
        send(wpart.at[:, cols], wpart.at[:, cols], S_WD, WD + n, sibling)
    wh_load.wait()
    blocks(1)
    zleaf(0)
    both = jnp.concatenate([inv, coef], axis=0)
    both = jnp.concatenate([both, jnp.zeros((6, T), F32)], axis=0).T
    own = (both[:, 0:1] * sgt_v[...] - both[:, 1:2] * ptt_v[...]).astype(BF16)
    for s in range(S):
        part_v[s] = dot(own, wst_v[:F, s * CS : (s + 1) * CS], ((1,), (0,)))
    zleaf(1)
    arrived(pgp_v, PG)
    for n in (0, 1):
        cols = pl.ds(pl.multiple_of((2 * n + 1 - core) * CS, 128), CS)
        arrived(wpart.at[:, cols], WD + n)
    for s in range(S):
        part_v[s] += dot(pgp_v[...], wst_v[F:, s * CS : (s + 1) * CS], ((0,), (0,)))
        ystep(0, s)
    blocks(2)
    blocks(3)
    zleaf(2)
    zleaf(3)
    for s in range(S):
        yown_cross(s)
    for s in (0, 1):
        ystep(1, s)
    for s in (2, 3):
        ystep(1, s)
    zjoin(6)
    zjoin(-6)
    for s in (0, 1):
        ystep(2, s)
    for s in (2, 3):
        ystep(2, s)
    zjoin(1)
    zjoin(-1)
    zjoin(4)
    zjoin(-4)
    for s in (0, 1):
        ystep(3, s)
    for s in (2, 3):
        ystep(3, s)
    for s in range(S):
        arrived(yfin.at[s], YF + s)
        own = part_v[s, pl.ds(yrows(0) + xl * 128, 16), :]
        for who, v, slots in ((xl, own, (0, 2)), (1 - xl, 0.0, (1, 3, 4))):
            for slot in slots:
                v = v + yfin[s, slot].astype(F32)
            cols = pl.ds(pl.multiple_of(who * HALF + s * CS, 128), CS)
            out_v[:, cols] = v.astype(BF16)

    v = joined(0)
    wg_v[:, :128] = v[:80]
    wg_v[:16, 128:] = v[80:96, :32]
    for j in (1, 2, 3):
        wg_v[16 * j : 16 * j + 16, 128:] = pltpu.roll(v[80:96], 128 - 32 * j, 1)[:, :32]
    wg_v[64:, 128:] = v[96:, :32]

    left(sums_v.at[: NT - 1], S_SUMS)
    left(wpart.at[:, : 2 * CS], S_WX)
    left(wpart.at[:, : 2 * CS], S_WD)
    left(pgp_v, S_PG)
    left(dsend, S_DD)
    left(zrecv, S_Z)
    left(yrecv, S_Y)
    left(yfin, S_YF)


def per_device(block_input, query_weight, query_gain, query_grad):
    hbm = pl.BlockSpec(memory_space=pltpu.HBM)
    vmem = pl.BlockSpec(memory_space=pltpu.VMEM)
    outs = (jax.ShapeDtypeStruct((T // NT, D), BF16), jax.ShapeDtypeStruct((80, F), F32))
    return pl.pallas_call(
        kernel,
        out_shape=outs,
        in_specs=[hbm, hbm, hbm, hbm],
        out_specs=(vmem, vmem),
        scratch_shapes=[
            pltpu.VMEM((T + F, D), BF16),
            pltpu.VMEM((NZ, 320, T), BF16),
            pltpu.VMEM((2 * F, HALF), BF16),
            pltpu.VMEM((1, F), F32),
            pltpu.VMEM((F, T), BF16),
            pltpu.VMEM((NT, 4, 128), F32),
            pltpu.VMEM((256, T), BF16),
            pltpu.VMEM((F, T), BF16),
            pltpu.VMEM((T, F), F32),
            pltpu.VMEM((T, F), F32),
            pltpu.VMEM((16, 2, PACK, 128), BF16),
            pltpu.VMEM((16, 2, PACK, 128), BF16),
            pltpu.VMEM((16, 2, PACK, 128), F32),
            pltpu.VMEM((16, 2, PACK, 128), BF16),
            pltpu.VMEM((NSLOT, PACK, 128), BF16),
            pltpu.VMEM((S, T, CS), F32),
            pltpu.VMEM((5, S, 32, CS), BF16),
            pltpu.VMEM((5, S, 32, CS), BF16),
            pltpu.VMEM((3, S, 32, CS), BF16),
            pltpu.VMEM((S, 5, 16, CS), BF16),
            pltpu.SemaphoreType.DMA((KC + 3,)),
            pltpu.SemaphoreType.DMA((8,)),
            pltpu.SemaphoreType.DMA((NRECV,)),
        ],
        compiler_params=pltpu.CompilerParams(
            collective_id=0, has_side_effects=True, vmem_limit_bytes=40 * 1024 * 1024
        ),
    )(*(pltpu.with_memory_space_constraint(a, pltpu.HBM) for a in (block_input, query_weight, query_gain.reshape(1, F), query_grad)))


def solution(mesh):
    return jax.shard_map(
        per_device,
        mesh=mesh,
        in_specs=(P("dp", None), P("tensor", None), P("tensor"), P("tensor", "dp")),
        out_specs=(P(("dp", "tensor"), None), P("dp", "tensor")),
        check_vma=False,
    )
```
